32 devices in a mesh: gx: 4 (over y, x), gy: 8 (over z, core).
Axes of the slice: x: 2, y: 2, z: 4, core: 2. Of those that a mesh axis runs over, the one named last changes fastest.
Arguments:
- velocity: float32 [2, 2048, 4096], P(None, 'gx', 'gy'), may hold values from -3 to 3
- stress: float32 [3, 2048, 4096], P(None, 'gx', 'gy'), may hold values from -3 to 3
- strength: float32 [2048, 4096], P('gx', 'gy'), may hold values from 0.5 to 4
- ice_mass: float32 [2048, 4096], P('gx', 'gy'), may hold values from 0.3 to 20, as said below
- wind_stress: float32 [2, 2048, 4096], P(None, 'gx', 'gy'), may hold values from -6 to 6
- current: float32 [2, 2048, 4096], P(None, 'gx', 'gy'), may hold values from -3 to 3
- ice_mask: int32 [2048, 4096], P('gx', 'gy'), may hold values from 0 to 1, as said below
- open_water: int32 [2048, 4096], P('gx', 'gy'), may hold values 0 or 1
Outputs:
- new_velocity: float32 [2, 2048, 4096], P(None, 'gx', 'gy')
- new_stress: float32 [3, 2048, 4096], P(None, 'gx', 'gy')
- residual: float32 [], replicated
- kinetic_energy: float32 [], replicated
The draws below stay inside these ranges and needn't reach their ends.
Inputs may be any that keep to these rules, and one draw needn't show every extreme that they name: `ice_mask`: 1 marks an ocean cell, 0 a land cell. `ice_mass`: positive everywhere.
All inputs are finite; a program needn't handle non-finite values. No bound on the sum of `open_water` on one device may be relied on, other than what follows from the above.
Results may differ from the reference program's by a relative error of at most 0.00002.
Values sent between devices are 32-bit elements; how exact they have to be, the bound alone decides.
A program may use at most 128 MiB of HBM per device.

```python
import math
import jax
import jax.numpy as jnp

ITERS = 4
NX = 2048
NY = 4096


def draw_ice_mass(key, part):
    row_ramp = 1.0 + 2.0 * jnp.arange(NX, dtype=jnp.float32) / NX
    col_ramp = 1.0 + 2.0 * jnp.arange(NY, dtype=jnp.float32) / NY
    ramp = row_ramp[:, None] * col_ramp[None, :]
    rough = jax.random.uniform(key, (NX, NY), jnp.float32, 0.6, 1.4)
    return (ramp * rough).astype(jnp.float32)


def draw_ice_mask(key, part):
    row_index = jnp.arange(NX, dtype=jnp.int32)[:, None]
    col_index = jnp.arange(NY, dtype=jnp.int32)[None, :]
    land_cells = jnp.zeros((NX, NY), jnp.int32)
    for number in range(8):
        key_a, key_b, key_c, key_d = jax.random.split(jax.random.fold_in(key, number + 11), 4)
        start_x = jax.random.randint(key_a, (), 0, NX)
        width_x = jax.random.randint(key_b, (), 1, max(NX // 4, 2))
        start_y = jax.random.randint(key_c, (), 0, NY)
        width_y = jax.random.randint(key_d, (), 1, max(NY // 4, 2))
        inside = (row_index >= start_x) & (row_index < start_x + width_x) & (col_index >= start_y) & (col_index < start_y + width_y)
        land_cells = jnp.maximum(land_cells, inside.astype(jnp.int32))
    speckle = (jax.random.randint(jax.random.fold_in(key, 97), (NX, NY), 0, 16) == 0).astype(jnp.int32)
    land_cells = jnp.maximum(land_cells, speckle)
    return (1 - land_cells).astype(jnp.int32)


def set_ends(entries, own_key, low, high):
    longest = entries.shape.index(max(entries.shape))
    spots = []
    for shift in (0, 1):
        where = [jax.random.randint(jax.random.fold_in(own_key, axis), (), 0, length) for axis, length in enumerate(entries.shape)]
        where[longest] = (where[longest] + shift) % entries.shape[longest]
        spots.append(tuple(where))
    return entries.at[spots[0]].set(low).at[spots[1]].set(high)


def levels(key, extent, shards, smallest, high):
    level, own = 1.0, jax.random.fold_in(key, 6)
    for dim, blocks in shards:
        heights = jnp.exp(jax.random.uniform(jax.random.fold_in(own, dim), (blocks,), jnp.float32, smallest / len(shards), high / len(shards)))
        level = level * jnp.repeat(heights, extent[dim] // blocks).reshape([-1 if axis == dim else 1 for axis in range(len(extent))])
    return level


def normal_values(rng, dims, deviation, most, cuts=(), kind=jnp.bfloat16):
    level = levels(rng, dims, cuts, -0.22, 0.18) if cuts else 1.0
    drawn = jax.random.normal(rng, dims, jnp.float32) * deviation * level
    return jnp.minimum(jnp.maximum(drawn, -most), most).astype(kind)


def setup_inputs(seed: int = 0) -> dict:
    key_of = jax.random.split(jax.random.key(seed), 9)
    velocity = normal_values(key_of[0], (2, NX, NY), 0.5, 3.0, ((1, 4), (2, 8)), jnp.float32)
    stress = normal_values(key_of[1], (3, NX, NY), 0.5, 3.0, ((1, 4), (2, 8)), jnp.float32)
    strength = jnp.clip(jnp.exp(math.log(4.0) - 2.0794415 * jax.random.uniform(key_of[2], (NX, NY), jnp.float32) ** levels(key_of[2], (NX, NY), ((0, 4), (1, 8)), -0.2, 0.2)), 0.5, 4.0)
    ice_mass = draw_ice_mass(jax.random.fold_in(key_of[8], 71), 0)
    wind_stress = normal_values(key_of[4], (2, NX, NY), 1.0, 6.0, ((1, 4), (2, 8)), jnp.float32)
    current = normal_values(key_of[5], (2, NX, NY), 0.5, 3.0, ((1, 4), (2, 8)), jnp.float32)
    ice_mask = draw_ice_mask(jax.random.fold_in(key_of[8], 71), 0)
    open_water = set_ends((jax.random.randint(key_of[7], (NX, NY), 0, 8) < 1).astype(jnp.int32), jax.random.fold_in(key_of[7], 1), 0, 1)
    return {"velocity": velocity, "stress": stress, "strength": strength, "ice_mass": ice_mass, "wind_stress": wind_stress, "current": current, "ice_mask": ice_mask, "open_water": open_water}


relax_rate = 0.8
ecc_square = 4.0
delta_floor = 0.05
time_step = 0.5
drag_coef = 1.0
coriolis = 0.3

def corner_diffs(values):
    along_x = (values[1:, 1:] + values[1:, :-1] - values[:-1, 1:] - values[:-1, :-1]) * 0.5
    along_y = (values[1:, 1:] + values[:-1, 1:] - values[1:, :-1] - values[:-1, :-1]) * 0.5
    return (along_x, along_y)

def update_stress(velocity, stress, pressure):
    du_dx, du_dy = corner_diffs(velocity[0])
    dv_dx, dv_dy = corner_diffs(velocity[1])
    divu = du_dx + dv_dy
    tension = du_dx - dv_dy
    shear = du_dy + dv_dx
    deform = jnp.sqrt(divu * divu + (tension * tension + shear * shear) / ecc_square + delta_floor * delta_floor)
    viscous = pressure / deform
    first = (stress[0] + relax_rate * viscous * (divu - deform)) / (1.0 + relax_rate)
    second = (stress[1] + relax_rate * viscous * tension / ecc_square) / (1.0 + relax_rate)
    third = (stress[2] + relax_rate * viscous * shear * 0.5 / ecc_square) / (1.0 + relax_rate)
    return jnp.stack([first, second, third])

def stress_force(stress):
    normal_x = 0.5 * (stress[0] + stress[1])
    normal_y = 0.5 * (stress[0] - stress[1])
    normal_x_dx, unused_x = corner_diffs(normal_x)
    unused_y, normal_y_dy = corner_diffs(normal_y)
    shear_dx, shear_dy = corner_diffs(stress[2])
    return (normal_x_dx + shear_dy, shear_dx + normal_y_dy)

def advance(velocity, force_x, force_y, ice_mass, wind_stress, current, ice_weight):
    inertia = ice_mass / time_step
    diagonal = inertia + drag_coef
    turning = ice_mass * coriolis
    rhs_u = inertia * velocity[0] + force_x + wind_stress[0] + drag_coef * current[0]
    rhs_v = inertia * velocity[1] + force_y + wind_stress[1] + drag_coef * current[1]
    determinant = diagonal * diagonal + turning * turning
    new_u = (diagonal * rhs_u + turning * rhs_v) / determinant * ice_weight
    new_v = (diagonal * rhs_v - turning * rhs_u) / determinant * ice_weight
    return jnp.stack([new_u, new_v])

def reference(velocity, stress, strength, ice_mass, wind_stress, current, ice_mask, open_water):
    ice_weight = ice_mask.astype(jnp.float32) * (1.0 - open_water.astype(jnp.float32))
    pressure = strength * ice_weight
    previous = velocity
    for subcycle in range(ITERS):
        padded = jnp.pad(velocity, ((0, 0), (1, 0), (1, 0)))
        stress = update_stress(padded, stress, pressure)
        force_x, force_y = stress_force(jnp.pad(stress, ((0, 0), (0, 1), (0, 1))))
        previous = velocity
        velocity = advance(velocity, force_x, force_y, ice_mass, wind_stress, current, ice_weight)
    change = velocity - previous
    residual = jnp.sum(ice_weight * (change[0] * change[0] + change[1] * change[1])) / (NX * NY)
    kinetic = 0.5 * jnp.sum(ice_mass * ice_weight * (velocity[0] * velocity[0] + velocity[1] * velocity[1])) / (NX * NY)
    return (velocity, stress, residual, kinetic)
```

```python
import functools

import jax
import jax.numpy as jnp
from jax import lax
from jax.experimental import pallas as pl
from jax.experimental.pallas import tpu as pltpu
from jax.sharding import PartitionSpec as P

ITERS = 4
relax_rate = 0.8
time_step = 0.5
drag_coef = 1.0
coriolis = 0.3
delta_floor = 0.05
MESH = pl.DeviceIdType.MESH

Q, R, QX, RX, AL, BE, S2 = range(7)
PR, M, TQ, TR, CA, CB = range(6)
SENT = ((0, Q), (0, R), (0, AL), (0, BE), (0, S2)) + tuple((1, f) for f in range(6))
NF = len(SENT)
PAIRS = (NF + 1) // 2
LANE = 128
PAD = 8
UN = 4
DIRS = ((-1, 0), (1, 0), (0, -1), (0, 1), (-1, -1), (-1, 1), (1, -1), (1, 1))
CORNERS = ((-1, 0), (1, 0)) + DIRS[4:]
f32 = jnp.float32


def iota(axis):
    return lax.broadcasted_iota(jnp.int32, (8, LANE), axis)


def roll(x, by, axis):
    by %= x.shape[axis]
    return pltpu.roll(x, by, axis=axis) if by else x


def here(k):
    return pl.ds(pl.multiple_of(k * 8 + PAD, 8), 8)


def near(k, off):
    return pl.ds(k * 8 + PAD + off, 8)


def shift(xs, by, first, last):
    n = len(xs)
    turned = [roll(x, by, 1) for x in xs]
    if by > 0:
        return [jnp.where(first, turned[(j - 1) % n], turned[j]) for j in range(n)]
    return [jnp.where(last, turned[(j + 1) % n], turned[j]) for j in range(n)]


class Sweep:
    def __init__(self, tiles, turned):
        self.n, self.turned = tiles, turned
        self.first, self.last = iota(1) == 0, iota(1) == LANE - 1

    def spread(self, st, k):
        for f in (Q, R):
            xs = shift([st[f, j, here(k), :] for j in range(self.n)], 1, self.first, self.last)
            for j, x in enumerate(xs):
                st[f + 2, j, here(k), :] = x

    def stress(self, old, new, par, k):
        at, up = here(k), near(k, -1)
        keep = 1.0 / (1.0 + relax_rate)
        for j in range(self.n):
            q, r, qx, rx = (old[f, j, at, :] for f in (Q, R, QX, RX))
            qa, ra, qxa, rxa = (old[f, j, up, :] for f in (Q, R, QX, RX))
            a, b = q - qxa, rx - ra
            if self.turned:
                d, s = a - b, a + b
                t = (r - rxa) - (qx - qa)
            else:
                d, s = a + b, a - b
                t = (r - rxa) + (qx - qa)
            e = (d * d + 4.0 * delta_floor * delta_floor) + 0.25 * (t * t + s * s)
            pr = par[PR, j, at, :]
            g = pr * lax.rsqrt(e)
            h = 0.25 * g
            push, side = g * d - pr, h * s
            new[AL, j, at, :] = old[AL, j, at, :] * keep + (push + side)
            new[BE, j, at, :] = old[BE, j, at, :] * keep + (push - side)
            new[S2, j, at, :] = old[S2, j, at, :] * keep + h * t

    def force(self, new, frc, k):
        at, dn = here(k), near(k, 1)
        a, c = [], []
        for j in range(self.n):
            ad, s, sd, b = new[AL, j, dn, :], new[S2, j, at, :], new[S2, j, dn, :], new[BE, j, at, :]
            if self.turned:
                a.append(ad + s)
                c.append(sd + b)
            else:
                a.append(ad - s)
                c.append(sd - b)
        for f, xs in ((0, a), (1, c)):
            for j, x in enumerate(shift(xs, -1, self.first, self.last)):
                frc[f, j, at, :] = x

    def velocity(self, old, new, frc, par, k, acc=None):
        at, dn = here(k), near(k, 1)
        out = []
        for j in range(self.n):
            al, s, sd, bd = new[AL, j, at, :], new[S2, j, at, :], new[S2, j, dn, :], new[BE, j, dn, :]
            fa, fc = frc[0, j, at, :], frc[1, j, at, :]
            if self.turned:
                fq, fr = fa - (sd + al), fc - (bd + s)
            else:
                fq, fr = fa + (sd - al), fc + (bd - s)
            q, r, m = old[Q, j, at, :], old[R, j, at, :], par[M, j, at, :]
            x = m * q + (fq + par[TQ, j, at, :])
            y = m * r + (fr + par[TR, j, at, :])
            ca, cb = par[CA, j, at, :], par[CB, j, at, :]
            nq, nr = ca * x - cb * y, ca * y + cb * x
            new[Q, j, at, :] = nq
            new[R, j, at, :] = nr
            out.append((nq, nr))
            if acc is not None:
                dq, dr = nq - q, nr - r
                acc(j, dq * dq + dr * dr, m * (nq * nq + nr * nr))
        if acc is None:
            for f in (0, 1):
                xs = shift([o[f] for o in out], 1, self.first, self.last)
                for j, x in enumerate(xs):
                    new[f + 2, j, at, :] = x


def main_sweep(sw, old, new, frc, par, blocks, final):
    n = sw.n
    trips = blocks // UN
    zero = jnp.zeros((8, LANE), f32)
    sums = (zero,) * (2 * n)

    def vel(ks, sums):
        sums = list(sums)

        def acc(j, x, y):
            sums[2 * j] += x
            sums[2 * j + 1] += y

        for k in ks:
            if not final:
                sw.velocity(old, new, frc, par, k)
            elif not isinstance(k, int) or 0 < k < blocks - 1:
                sw.velocity(old, new, frc, par, k, acc)
        return tuple(sums)

    for k in range(UN):
        sw.stress(old, new, par, k)
    for k in range(UN - 1):
        sw.force(new, frc, k)
    for k in range(UN, 2 * UN):
        sw.stress(old, new, par, k)
    sums = vel(range(UN - 1), sums)
    for k in range(UN - 1, 2 * UN - 1):
        sw.force(new, frc, k)
    for k in range(2 * UN, 3 * UN):
        sw.stress(old, new, par, k)

    def body(p, sums):
        sums = vel([UN * (p - 2) - 1 + i for i in range(UN)], sums)
        for i in range(UN):
            sw.force(new, frc, UN * (p - 1) - 1 + i)
        for i in range(UN):
            sw.stress(old, new, par, UN * p + i)
        return sums

    sums = lax.fori_loop(3, trips, body, sums)
    sums = vel([blocks - UN - 1 - UN + i for i in range(UN)], sums)
    for i in range(UN + 1):
        sw.force(new, frc, blocks - UN - 1 + i)
    return vel([blocks - UN - 1 + i for i in range(UN + 1)], sums)


def core_kernel(
    nx, ny, rows, cols,
    vel, stress, strength, mass, wind, current, mask, water,
    vel_out, stress_out, total_out,
    strength_v, mass_v, mask_v, water_v, vel_v, stress_v, wind_v, current_v,
    st_a, st_b, frc, par,
    pack_u, pack_d, recv_u, recv_d, own_l, own_r, recv_l, recv_r,
    corner_u, corner_d, corner_in,
    row_a, row_b, row_f, row_p, col_a, col_b, col_f, col_p,
    packed, edge_t, edge, mine, slots,
    load_sem, send_sem, recv_sem, sum_send, sum_recv,
):
    ix = lax.axis_index("gx")
    iy = lax.axis_index("gy")
    n, tall, blocks = cols // LANE, rows // LANE, rows // 8
    chunks = 8
    per = rows // chunks
    lane, sub = iota(1), iota(0)
    zero = jnp.zeros((8, LANE), f32)

    def loads(c):
        part = pl.ds(c * per, per)
        both = slice(None)
        pairs = (
            (strength.at[part], strength_v.at[part]),
            (mass.at[part], mass_v.at[part]),
            (mask.at[part], mask_v.at[part]),
            (water.at[part], water_v.at[part]),
            (vel.at[both, part], vel_v.at[both, part]),
            (stress.at[both, part], stress_v.at[both, part]),
            (wind.at[both, part], wind_v.at[both, part]),
            (current.at[both, part], current_v.at[both, part]),
        )
        return [pltpu.make_async_copy(a, b, load_sem.at[c, k]) for k, (a, b) in enumerate(pairs)]

    for c in [0, chunks - 1] + list(range(1, chunks - 1)):
        for cp in loads(c):
            cp.start()

    count = nx * ny
    me = ix * ny + iy

    def target(k):
        t = lax.rem(me + k, count)
        return (t // ny, lax.rem(t, ny))

    barrier = pltpu.get_barrier_semaphore()

    def greet(k, c):
        pl.semaphore_signal(barrier, inc=1, device_id=target(k), device_id_type=MESH)
        return c

    lax.fori_loop(1, count, greet, 0)

    for st in (st_a, st_b):
        for f in range(7):
            for j in range(n):
                st[f, j, 0:8, :] = zero
                st[f, j, rows + PAD : rows + 16, :] = zero
    for st in (row_a, row_b, col_a, col_b):
        for side in range(2):
            for f in range(7):
                for j in range(st.shape[2]):
                    st[side, f, j, 0:8, :] = zero
                    st[side, f, j, 24:32, :] = zero

    sw = Sweep(n, False)

    def prepare(k):
        rowsl = pl.ds(pl.multiple_of(k * 8, 8), 8)
        at = here(k)
        qs, rs = [], []
        ends = []
        for j in range(n):
            src = (rowsl, slice(j * LANE, (j + 1) * LANE))
            w = mask_v[src].astype(f32) * (1.0 - water_v[src].astype(f32))
            m = mass_v[src]
            inertia = m * (1.0 / time_step)
            diagonal = inertia + drag_coef
            turning = m * coriolis
            scale = (0.5 * w) / (diagonal * diagonal + turning * turning)
            tx = wind_v[(0,) + src] + drag_coef * current_v[(0,) + src]
            ty = wind_v[(1,) + src] + drag_coef * current_v[(1,) + src]
            u, v = vel_v[(0,) + src], vel_v[(1,) + src]
            s1, s2, s12 = (stress_v[(i,) + src] for i in range(3))
            t = s12 + s12
            q, r = u + v, u - v
            state = {Q: q, R: r, AL: s1 + t, BE: s1 - t, S2: s2}
            fixed = {
                PR: strength_v[src] * w * (relax_rate / (1.0 + relax_rate)),
                M: inertia * 2.0,
                TQ: (tx + ty) * 2.0,
                TR: (tx - ty) * 2.0,
                CA: diagonal * scale,
                CB: turning * scale,
            }
            for f, x in state.items():
                st_a[f, j, at, :] = x
            for f, x in fixed.items():
                par[f, j, at, :] = x
            qs.append(q)
            rs.append(r)
            if j in (0, n - 1):
                ends.append([(state, fixed)[a][f] for a, f in SENT])
        for f, xs in ((QX, qs), (RX, rs)):
            for j, x in enumerate(shift(xs, 1, sw.first, sw.last)):
                st_a[f, j, at, :] = x
        low, high = ends[0], ends[-1]
        packs = [zero, zero]
        for i in range(NF):
            x = roll(jnp.where(lane < LANE // 2, low[i], high[i]), 16 * (i % 8) + 8, 1)
            g = lane // 16 == i % 8
            packs[i // 8] = jnp.where(g, x, packs[i // 8])
        for i in range(2):
            packed[i, rowsl, :] = packs[i]

    def prepare_chunk(c):
        for cp in loads(c):
            cp.wait()

        def body(k, carry):
            prepare(k)
            return carry

        lax.fori_loop(c * (per // 8), (c + 1) * (per // 8), body, 0)

    def exists(d):
        return (ix + d[0] >= 0) & (ix + d[0] < nx) & (iy + d[1] >= 0) & (iy + d[1] < ny)

    def message(d, which):
        k = DIRS.index(d)
        dx, dy = d
        out = []
        if which == 1:
            pass
        elif dy == 0:
            out.append((pack_u, recv_d, k) if dx < 0 else (pack_d, recv_u, k))
        elif dx == 0:
            out.append((own_l, recv_r, k) if dy < 0 else (own_r, recv_l, k))
        if dx and which != 0:
            c = CORNERS.index(d)
            back = CORNERS.index((-dx, -dy))
            out.append((corner_u if dx < 0 else corner_d, corner_in.at[back], 4 + c))
        return [
            pltpu.make_async_remote_copy(
                src_ref=a, dst_ref=b, send_sem=send_sem.at[s], recv_sem=recv_sem.at[s],
                device_id=(ix + dx, iy + dy), device_id_type=MESH,
            )
            for a, b, s in out
        ]

    def plane(i):
        a, f = SENT[i]
        return (st_a, par)[a], f

    prepare_chunk(0)
    prepare_chunk(chunks - 1)
    top, bottom = slice(PAD, PAD + 8), slice(rows, rows + 8)
    for g in range(PAIRS):
        i0, i1 = 2 * g, min(2 * g + 1, NF - 1)
        (a0, f0), (a1, f1) = plane(i0), plane(i1)
        for j in range(n):
            pack_u[g, j] = jnp.where(sub < 4, a0[f0, j, top, :], roll(a1[f1, j, top, :], 4, 0))
            pack_d[g, j] = jnp.where(sub < 4, roll(a0[f0, j, bottom, :], 4, 0), a1[f1, j, bottom, :])
    pl.semaphore_wait(barrier, count - 1)
    for d in DIRS[:2]:
        @pl.when(exists(d))
        def _():
            message(d, 0)[0].start()

    for c in range(1, chunks - 1):
        prepare_chunk(c)

    for i in range(2):
        for t in range(tall):
            x = packed[i, t * LANE : (t + 1) * LANE, :].T
            for f in range(8 * i, min(8 * i + 8, NF)):
                o = 16 * (f - 8 * i)
                own_r[f, t] = x[o : o + 8]
                own_l[f, t] = x[o + 8 : o + 16]
                a, g = SENT[f]
                dst = (col_a, col_p)[a]
                dst[0, g, t, 16:24, :] = x[o + 8 : o + 16]
                dst[1, g, t, 8:16, :] = x[o : o + 8]
    up, down = zero, zero
    for i in range(2 * NF):
        src = own_l if i < NF else own_r
        g = lane // 4 == i
        up = jnp.where(g, roll(src[i % NF, 0], 4 * i, 1), up)
        down = jnp.where(g, roll(src[i % NF, tall - 1], 4 * i + 4, 1), down)
    corner_u[...] = up
    corner_d[...] = down
    for d in DIRS[2:4]:
        @pl.when(exists(d))
        def _():
            message(d, 0)[0].start()
    for d in CORNERS:
        @pl.when(exists(d))
        def _():
            message(d, 1)[0].start()

    for i in range(NF):
        a, f = SENT[i]
        src, g = plane(i)
        dst = (row_a, row_p)[a]
        for j in range(n):
            x, y = (roll(src[g, j, b * 8 + PAD : b * 8 + PAD + 8, :], 4, 0) for b in (0, 1))
            dst[0, f, j, 8:16, :] = x
            dst[0, f, j, 16:24, :] = jnp.where(sub < 4, x, y)
            x, y = (roll(src[g, j, b * 8 + PAD : b * 8 + PAD + 8, :], 4, 0) for b in (blocks - 2, blocks - 1))
            dst[1, f, j, 8:16, :] = jnp.where(sub < 4, x, y)
            dst[1, f, j, 16:24, :] = y

    main_sweep(sw, st_a, st_b, frc, par, blocks, False)
    main_sweep(sw, st_b, st_a, frc, par, blocks, False)

    def clear(ref, lead):
        for i in lead:
            ref[i] = jnp.zeros(ref.shape[1:], f32)

    for d, buf in (((-1, 0), recv_u), ((1, 0), recv_d), ((0, -1), recv_l), ((0, 1), recv_r)):
        @pl.when(~exists(d))
        def _():
            clear(buf, range(buf.shape[0]))

    for c, d in enumerate(CORNERS):
        @pl.when(~exists(d))
        def _():
            corner_in[c] = zero

    for d in DIRS:
        @pl.when(exists(d))
        def _():
            for cp in message((-d[0], -d[1]), 2):
                cp.wait_recv()
            for cp in message(d, 2):
                cp.wait_send()

    for i in range(NF):
        a, f = SENT[i]
        dst = (row_a, row_p)[a]
        g, odd = divmod(i, 2)
        for j in range(n):
            x, y = recv_u[g, j], recv_d[g, j]
            x = roll(x, 4, 0) if odd else x
            y = y if odd else roll(y, 4, 0)
            dst[0, f, j, 8:16, :] = jnp.where(sub < 4, x, dst[0, f, j, 8:16, :])
            dst[1, f, j, 16:24, :] = jnp.where(sub < 4, dst[1, f, j, 16:24, :], y)
        dst = (col_a, col_p)[a]
        for t in range(tall):
            dst[0, f, t, 8:16, :] = recv_l[i, t]
            dst[1, f, t, 16:24, :] = recv_r[i, t]

        def corner(u, d, at):
            x = roll(corner_in[CORNERS.index(u)], LANE - 4 - 4 * at, 1)
            y = roll(corner_in[CORNERS.index(d)], -4 * at, 1)
            return jnp.where(lane < 4, y, jnp.where(lane >= LANE - 4, x, 0.0))

        dst[0, f, tall, 8:16, :] = corner((-1, -1), (1, -1), NF + i)
        dst[0, f, tall, 16:24, :] = corner((-1, 0), (1, 0), i)
        dst[1, f, tall, 8:16, :] = corner((-1, 0), (1, 0), NF + i)
        dst[1, f, tall, 16:24, :] = corner((-1, 1), (1, 1), i)

    strips = [
        (s, a.at[side], b.at[side], fr.at[side], p.at[side], side)
        for s, a, b, fr, p in (
            (sw, row_a, row_b, row_f, row_p),
            (Sweep(tall + 1, True), col_a, col_b, col_f, col_p),
        )
        for side in range(2)
    ]
    for s, a, b, fr, p, _ in strips:
        for k in range(2):
            s.spread(a, k)
    sums = [[zero, zero] for _ in range(n)]
    more = [zero, zero]
    for cyc in range(ITERS):
        final = cyc == ITERS - 1
        flip = cyc % 2
        for s, a, b, fr, p, _ in strips:
            old, new = (b, a) if flip else (a, b)
            for k in range(2):
                s.stress(old, new, p, k)
        for s, a, b, fr, p, _ in strips:
            new = a if flip else b
            for k in range(2):
                s.force(new, fr, k)
        for s, a, b, fr, p, side in strips:
            old, new = (b, a) if flip else (a, b)
            for k in range(2):
                if not final:
                    s.velocity(old, new, fr, p, k)
                    continue

                def acc(j, x, y):
                    if s.turned and (j == tall or k == side):
                        return
                    good = sub >= 4 if (k == 0) else sub < 4
                    box = more if s.turned else sums[j]
                    box[0] += jnp.where(good, x, 0.0)
                    box[1] += jnp.where(good, y, 0.0)

                s.velocity(old, new, fr, p, k, acc)
    row_e, col_e = (row_a, col_a) if ITERS % 2 == 0 else (row_b, col_b)

    main_sweep(sw, st_a, st_b, frc, par, blocks, False)
    inner = main_sweep(sw, st_b, st_a, frc, par, blocks, True)

    for j in range(n):
        good = lane >= 4 if j == 0 else lane < LANE - 4 if j == n - 1 else None
        if n == 1:
            good = (lane >= 4) & (lane < LANE - 4)
        for i in range(2):
            x = inner[2 * j + i] + sums[j][i]
            more[i] += x if good is None else jnp.where(good, x, 0.0)
    x, y = (jnp.sum(m, axis=0, keepdims=True) for m in more)
    x, y = x + roll(x, LANE // 2, 1), y + roll(y, LANE // 2, 1)
    half = lax.broadcasted_iota(jnp.int32, (1, LANE), 1) < LANE // 2
    part = jnp.where(half, x, y)
    mine[...] = part

    def sum_copy(k):
        return pltpu.make_async_remote_copy(
            src_ref=mine, dst_ref=slots.at[me], send_sem=sum_send.at[k], recv_sem=sum_recv.at[k],
            device_id=target(k), device_id_type=MESH,
        )

    def start(k, c):
        sum_copy(k).start()
        return c

    lax.fori_loop(1, count, start, 0)
    slots[pl.ds(me, 1)] = part[None]

    for t in range(tall):
        for o, f in enumerate((Q, R, AL, BE, S2)):
            x = jnp.where(sub < 4, col_e[0, f, t, 16:24, :], col_e[1, f, t, 8:16, :])
            edge_t[o * 8 : o * 8 + 8, :] = roll(x, 4, 0)
        edge[t * LANE : (t + 1) * LANE, :] = edge_t[...].T

    def emit(k, row, src, at):
        rowsl = pl.ds(row, 8)
        ev = edge[rowsl, :]
        es = [roll(ev, LANE - 4 - 8 * o, 1) for o in range(5)]
        for j in range(n):
            vals = [src[f, j, at, :] for f in (Q, R, AL, BE, S2)]
            if j == 0:
                vals = [jnp.where(lane < 4, e, x) for e, x in zip(es, vals)]
            if j == n - 1:
                vals = [jnp.where(lane >= LANE - 4, e, x) for e, x in zip(es, vals)]
            q, r, al, be, s2 = vals
            c = slice(j * LANE, (j + 1) * LANE)
            vel_out[0, rowsl, c] = 0.5 * (q + r)
            vel_out[1, rowsl, c] = 0.5 * (q - r)
            stress_out[0, rowsl, c] = 0.5 * (al + be)
            stress_out[1, rowsl, c] = s2
            stress_out[2, rowsl, c] = 0.25 * (al - be)

    emit(0, 0, row_e.at[0], slice(12, 20))
    emit(blocks - 1, rows - 8, row_e.at[1], slice(12, 20))

    def body(k, c):
        emit(k, pl.multiple_of(k * 8, 8), st_a, here(k))
        return c

    lax.fori_loop(1, blocks - 1, body, 0)

    def wait(k, c):
        sum_copy(k).wait()
        return c

    lax.fori_loop(1, count, wait, 0)
    total = slots[0]
    for i in range(1, count):
        total = total + slots[i]
    scale = 1.0 / (rows * nx * cols * ny)
    x = jnp.sum(jnp.where(half, total, 0.0), axis=1, keepdims=True) * (0.5 * scale)
    y = jnp.sum(jnp.where(half, 0.0, total), axis=1, keepdims=True) * (0.0625 * scale)
    total_out[...] = jnp.where(half, x, y)


def write_kernel(vel, stress, new_vel, new_stress, sem):
    copies = [
        pltpu.make_async_copy(vel, new_vel, sem.at[0]),
        pltpu.make_async_copy(stress, new_stress, sem.at[1]),
    ]
    for c in copies:
        c.start()
    for c in copies:
        c.wait()


def per_device(nx, ny, velocity, stress, strength, ice_mass, wind, current, ice_mask, open_water):
    _, rows, cols = velocity.shape
    n, tall, strip = cols // LANE, rows // LANE, rows + 2 * PAD
    i32 = jnp.int32
    vmem = pl.BlockSpec(memory_space=pltpu.VMEM)
    hbm = pl.BlockSpec(memory_space=pl.ANY)
    dma = pltpu.SemaphoreType.DMA
    V = pltpu.VMEM
    count = nx * ny
    new_vel, new_stress, total = pl.pallas_call(
        functools.partial(core_kernel, nx, ny, rows, cols),
        out_shape=(V((2, rows, cols), f32), V((3, rows, cols), f32), V((1, LANE), f32)),
        in_specs=[pl.BlockSpec(memory_space=pltpu.HBM)] * 8,
        out_specs=(vmem, vmem, vmem),
        scratch_shapes=[
            V((rows, cols), f32), V((rows, cols), f32), V((rows, cols), i32), V((rows, cols), i32),
            V((2, rows, cols), f32), V((3, rows, cols), f32), V((2, rows, cols), f32), V((2, rows, cols), f32),
            V((7, n, strip, LANE), f32), V((7, n, strip, LANE), f32),
            V((2, n, strip, LANE), f32), V((6, n, strip, LANE), f32),
            V((PAIRS, n, 8, LANE), f32), V((PAIRS, n, 8, LANE), f32),
            V((PAIRS, n, 8, LANE), f32), V((PAIRS, n, 8, LANE), f32),
            V((NF, tall, 8, LANE), f32), V((NF, tall, 8, LANE), f32),
            V((NF, tall, 8, LANE), f32), V((NF, tall, 8, LANE), f32),
            V((8, LANE), f32), V((8, LANE), f32), V((6, 8, LANE), f32),
            V((2, 7, n, 32, LANE), f32), V((2, 7, n, 32, LANE), f32),
            V((2, 2, n, 32, LANE), f32), V((2, 6, n, 32, LANE), f32),
            V((2, 7, tall + 1, 32, LANE), f32), V((2, 7, tall + 1, 32, LANE), f32),
            V((2, 2, tall + 1, 32, LANE), f32), V((2, 6, tall + 1, 32, LANE), f32),
            V((2, rows, LANE), f32), V((LANE, LANE), f32), V((rows, LANE), f32),
            V((1, LANE), f32), V((count, 1, LANE), f32),
            dma((8, 8)), dma((10,)), dma((10,)), dma((count,)), dma((count,)),
        ],
        compiler_params=pltpu.CompilerParams(
            collective_id=0, has_side_effects=True, vmem_limit_bytes=48 << 20
        ),
        name="core",
    )(
        *[
            pltpu.with_memory_space_constraint(x, pltpu.HBM)
            for x in (velocity, stress, strength, ice_mass, wind, current, ice_mask, open_water)
        ]
    )
    new_vel, new_stress = pl.pallas_call(
        write_kernel,
        out_shape=(
            jax.ShapeDtypeStruct(velocity.shape, f32),
            jax.ShapeDtypeStruct(stress.shape, f32),
        ),
        in_specs=[vmem, vmem],
        out_specs=(hbm, hbm),
        scratch_shapes=[dma((2,))],
        compiler_params=pltpu.CompilerParams(vmem_limit_bytes=8 << 20),
        name="write",
    )(new_vel, new_stress)
    return new_vel, new_stress, total[0, 0], total[0, LANE - 1]


def solution(mesh):
    two, three = P("gx", "gy"), P(None, "gx", "gy")
    return jax.shard_map(
        functools.partial(per_device, mesh.shape["gx"], mesh.shape["gy"]),
        mesh=mesh,
        in_specs=(three, three, two, two, three, three, two, two),
        out_specs=(three, three, P(), P()),
        check_vma=False,
    )
```

```python
import functools

import jax
import jax.numpy as jnp
from jax import lax
from jax.experimental import pallas as pl
from jax.experimental.pallas import tpu as pltpu
from jax.sharding import PartitionSpec as P

ITERS = 4
relax_rate = 0.8
time_step = 0.5
drag_coef = 1.0
coriolis = 0.3
delta_floor = 0.05
MESH = pl.DeviceIdType.MESH

Q, R = range(2)
AL, BE, S2 = range(3)
PR, M, TQ, TR, CA, CB = range(6)
SENT = ((0, Q), (0, R), (1, AL), (1, BE), (1, S2)) + tuple((2, f) for f in range(6))
NF = len(SENT)
PAIRS = (NF + 1) // 2
LANE = 128
PAD = 8
FRONT = 128
UN = 4
DIRS = ((-1, 0), (1, 0), (0, -1), (0, 1), (-1, -1), (-1, 1), (1, -1), (1, 1))
CORNERS = ((-1, 0), (1, 0)) + DIRS[4:]
f32 = jnp.float32


def iota(axis):
    return lax.broadcasted_iota(jnp.int32, (8, LANE), axis)


def roll(x, by, axis):
    by %= x.shape[axis]
    return pltpu.roll(x, by, axis=axis) if by else x


def rows8(row):
    if isinstance(row, int):
        return slice(row, row + 8)
    base, off = row
    return pl.ds(base + off if off % 8 else pl.multiple_of(base + off, 8), 8)


def select(mask, x, y):
    return lax.select(mask, x, y)


def shift(xs, by, first, last):
    n = len(xs)
    turned = [roll(x, by, 1) for x in xs]
    if by > 0:
        return [select(first, turned[(j - 1) % n], turned[j]) for j in range(n)]
    return [select(last, turned[(j + 1) % n], turned[j]) for j in range(n)]


class View:
    def __init__(self, ref, pad=PAD, base=None):
        self.ref, self.pad, self.base = ref, pad, base

    def at(self, i, off=0):
        row = self.pad + 8 * i + off
        return rows8(row if self.base is None else (self.base, row))

    def load(self, f, j, i, off=0):
        return self.ref[f, j, self.at(i, off), :]

    def store(self, f, j, i, x):
        self.ref[f, j, self.at(i), :] = x


class Sweep:
    def __init__(self, tiles, turned):
        self.n, self.turned = tiles, turned
        self.first, self.last = iota(1) == 0, iota(1) == LANE - 1

    def spread(self, ve, vx, i):
        for f in (Q, R):
            xs = shift([ve.load(f, j, i) for j in range(self.n)], 1, self.first, self.last)
            for j, x in enumerate(xs):
                vx.store(f, j, i, x)

    def stress(self, ve, vx, old, new, par, i):
        keep = 1.0 / (1.0 + relax_rate)
        for j in range(self.n):
            q, r, qx, rx = (v.load(f, j, i) for v in (ve, vx) for f in (Q, R))
            qa, ra, qxa, rxa = (v.load(f, j, i, -1) for v in (ve, vx) for f in (Q, R))
            a, b = q - qxa, rx - ra
            if self.turned:
                d, s = a - b, a + b
                t = (r - rxa) - (qx - qa)
            else:
                d, s = a + b, a - b
                t = (r - rxa) + (qx - qa)
            e = (d * d + 4.0 * delta_floor * delta_floor) + 0.25 * (t * t + s * s)
            pr = par.load(PR, j, i)
            g = pr * lax.rsqrt(e)
            h = 0.25 * g
            push, side = g * d - pr, h * s
            new.store(AL, j, i, old.load(AL, j, i) * keep + (push + side))
            new.store(BE, j, i, old.load(BE, j, i) * keep + (push - side))
            new.store(S2, j, i, old.load(S2, j, i) * keep + h * t)

    def force(self, ss, frc, i):
        a, c = [], []
        for j in range(self.n):
            ad, s, sd, b = ss.load(AL, j, i, 1), ss.load(S2, j, i), ss.load(S2, j, i, 1), ss.load(BE, j, i)
            if self.turned:
                a.append(ad + s)
                c.append(sd + b)
            else:
                a.append(ad - s)
                c.append(sd - b)
        for f, xs in ((0, a), (1, c)):
            for j, x in enumerate(shift(xs, -1, self.first, self.last)):
                frc.store(f, j, i, x)

    def velocity(self, old, new, ss, frc, par, i):
        for j in range(self.n):
            al, s, sd, bd = ss.load(AL, j, i), ss.load(S2, j, i), ss.load(S2, j, i, 1), ss.load(BE, j, i, 1)
            fa, fc = frc.load(0, j, i), frc.load(1, j, i)
            if self.turned:
                fq, fr = fa - (sd + al), fc - (bd + s)
            else:
                fq, fr = fa + (sd - al), fc + (bd - s)
            q, r, m = old.load(Q, j, i), old.load(R, j, i), par.load(M, j, i)
            x = m * q + (fq + par.load(TQ, j, i))
            y = m * r + (fr + par.load(TR, j, i))
            ca, cb = par.load(CA, j, i), par.load(CB, j, i)
            new.store(Q, j, i, ca * x - cb * y)
            new.store(R, j, i, ca * y + cb * x)

    def reduce(self, old, new, par, i, add):
        for j in range(self.n):
            nq, nr = new.load(Q, j, i), new.load(R, j, i)
            dq, dr = nq - old.load(Q, j, i), nr - old.load(R, j, i)
            add(j, dq * dq + dr * dr, par.load(M, j, i) * (nq * nq + nr * nr))


class Stream:
    def __init__(self, sw, ve, vx, ss, frc, par, rows):
        self.sw, self.ve, self.vx, self.ss, self.frc, self.par, self.rows = sw, ve, vx, ss, frc, par, rows

    def base(self, p, lag, mod):
        x = p * (8 * UN) - 8 * UN * lag
        return pl.multiple_of(lax.rem(x + (lag * mod if lag else 0), mod), 8 * UN)

    def step(self, p, stages):
        sw, rows, unit = self.sw, self.rows, 8 * UN
        row = pl.multiple_of(p * unit, unit)
        ss = [View(self.ss, PAD, self.base(p, lag, rows)) for lag in (0, 2, 3)]
        par = [View(self.par, PAD, self.base(p, lag, rows)) for lag in (0, 3)]
        slots = [View(self.frc, PAD, pl.multiple_of(lax.rem(p + k, 2) * unit, unit)) for k in (0, 1)]
        was = lambda lag: View(self.ve, FRONT - lag * unit, row)
        now = lambda lag: View(self.ve, FRONT + rows - lag * unit, row)
        vx = View(self.vx, PAD, self.base(p, 0, 2 * rows))
        shifted = View(self.vx, PAD, pl.multiple_of(lax.rem(row + 3 * rows - 4 * unit, 2 * rows), unit))
        todo = {
            "velocity": (was(3), now(3), ss[2], slots[1], par[1]),
            "force": (ss[1], slots[0]),
            "stress": (was(0), vx, ss[0], ss[0], par[0]),
            "spread": (now(4), shifted),
        }
        for name in stages:
            for i in range(UN):
                getattr(sw, name)(*todo[name], i)

    def run(self):
        steps = ITERS * self.rows // (8 * UN)
        every = ("velocity", "force", "stress", "spread")
        parts = (
            (0, 2, every[2:3]), (2, 3, every[1:3]), (3, 4, every[:3]),
            (4, steps, every), (steps, steps + 3, every[:2]),
        )
        for lo, hi, stages in parts:
            def body(p, carry):
                self.step(p, stages)
                return carry

            lax.fori_loop(lo, hi, body, 0)


def core_kernel(
    nx, ny, rows, cols,
    vel, stress, strength, mass, wind, current, mask, water,
    vel_out, stress_out, total_out,
    strength_v, mass_v, mask_v, water_v, vel_v, stress_v, wind_v, current_v,
    ve, vx, ss, frc, par, acc,
    pack_u, pack_d, recv_u, recv_d, own_l, own_r, recv_l, recv_r,
    corner_u, corner_d, corner_in,
    row_va, row_vb, row_sa, row_sb, row_x, row_f, row_p, col_va, col_vb, col_sa, col_sb, col_x, col_f, col_p,
    packed, edge_t, edge, mine, slots,
    load_sem, send_sem, recv_sem, sum_send, sum_recv,
):
    ix = lax.axis_index("gx")
    iy = lax.axis_index("gy")
    n, tall, blocks = cols // LANE, rows // LANE, rows // 8
    chunks = 8
    per = rows // chunks
    lane, sub = iota(1), iota(0)
    zero = jnp.zeros((8, LANE), f32)

    def loads(c):
        part = pl.ds(c * per, per)
        both = slice(None)
        pairs = (
            (strength.at[part], strength_v.at[part]),
            (mass.at[part], mass_v.at[part]),
            (mask.at[part], mask_v.at[part]),
            (water.at[part], water_v.at[part]),
            (vel.at[both, part], vel_v.at[both, part]),
            (stress.at[both, part], stress_v.at[both, part]),
            (wind.at[both, part], wind_v.at[both, part]),
            (current.at[both, part], current_v.at[both, part]),
        )
        return [pltpu.make_async_copy(a, b, load_sem.at[c, k]) for k, (a, b) in enumerate(pairs)]

    for c in [0, chunks - 1] + list(range(1, chunks - 1)):
        for cp in loads(c):
            cp.start()

    count = nx * ny
    me = ix * ny + iy

    def target(k):
        t = lax.rem(me + k, count)
        return (t // ny, lax.rem(t, ny))

    barrier = pltpu.get_barrier_semaphore()

    def greet(k, c):
        pl.semaphore_signal(barrier, inc=1, device_id=target(k), device_id_type=MESH)
        return c

    lax.fori_loop(1, count, greet, 0)

    for j in range(n):
        for f in range(2):
            ve[f, j, FRONT - 8 : FRONT, :] = zero
            vx[f, j, 0:8, :] = zero
        for f in range(3):
            ss[f, j, rows + PAD : rows + 16, :] = zero
    for st in (row_va, row_vb, row_sa, row_sb, row_x, col_va, col_vb, col_sa, col_sb, col_x):
        for side in range(2):
            for f in range(st.shape[1]):
                for j in range(st.shape[2]):
                    st[side, f, j, 0:8, :] = zero
                    st[side, f, j, 24:32, :] = zero

    sw = Sweep(n, False)

    def prepare(base, i):
        rowsl, at = rows8((base, 8 * i)), rows8((base, 8 * i + PAD))
        first = rows8((base, 8 * i + FRONT))
        ends = []
        for j in range(n):
            src = (rowsl, slice(j * LANE, (j + 1) * LANE))
            w = mask_v[src].astype(f32) * (1.0 - water_v[src].astype(f32))
            m = mass_v[src]
            inertia = m * (1.0 / time_step)
            diagonal = inertia + drag_coef
            turning = m * coriolis
            scale = (0.5 * w) / (diagonal * diagonal + turning * turning)
            tx = wind_v[(0,) + src] + drag_coef * current_v[(0,) + src]
            ty = wind_v[(1,) + src] + drag_coef * current_v[(1,) + src]
            u, v = vel_v[(0,) + src], vel_v[(1,) + src]
            s1, s2, s12 = (stress_v[(i,) + src] for i in range(3))
            t = s12 + s12
            q, r = u + v, u - v
            moving = {Q: q, R: r}
            state = {AL: s1 + t, BE: s1 - t, S2: s2}
            fixed = {
                PR: strength_v[src] * w * (relax_rate / (1.0 + relax_rate)),
                M: inertia * 2.0,
                TQ: (tx + ty) * 2.0,
                TR: (tx - ty) * 2.0,
                CA: diagonal * scale,
                CB: turning * scale,
            }
            for f, x in moving.items():
                ve[f, j, first, :] = x
            for f, x in state.items():
                ss[f, j, at, :] = x
            for f, x in fixed.items():
                par[f, j, at, :] = x
            if j in (0, n - 1):
                ends.append([(moving, state, fixed)[a][f] for a, f in SENT])
        low, high = ends[0], ends[-1]
        packs = [zero, zero]
        for i in range(NF):
            x = roll(select(lane < LANE // 2, low[i], high[i]), 16 * (i % 8) + 8, 1)
            g = (lane >= 16 * (i % 8)) & (lane < 16 * (i % 8) + 16)
            packs[i // 8] = select(g, x, packs[i // 8])
        for i in range(2):
            packed[i, rowsl, :] = packs[i]

    def prepare_chunk(c):
        for cp in loads(c):
            cp.wait()

        group = min(UN, per // 8)

        def body(p, carry):
            base = pl.multiple_of(p * (8 * group), 8 * group)
            for i in range(group):
                prepare(base, i)
            for i in range(group):
                sw.spread(View(ve, FRONT, base), View(vx, PAD, base), i)
            return carry

        lax.fori_loop(c * (per // 8) // group, (c + 1) * (per // 8) // group, body, 0)

    def exists(d):
        return (ix + d[0] >= 0) & (ix + d[0] < nx) & (iy + d[1] >= 0) & (iy + d[1] < ny)

    def message(d, which):
        k = DIRS.index(d)
        dx, dy = d
        out = []
        if which == 1:
            pass
        elif dy == 0:
            out.append((pack_u, recv_d, k) if dx < 0 else (pack_d, recv_u, k))
        elif dx == 0:
            out.append((own_l, recv_r, k) if dy < 0 else (own_r, recv_l, k))
        if dx and which != 0:
            c = CORNERS.index(d)
            back = CORNERS.index((-dx, -dy))
            out.append((corner_u if dx < 0 else corner_d, corner_in.at[back], 4 + c))
        return [
            pltpu.make_async_remote_copy(
                src_ref=a, dst_ref=b, send_sem=send_sem.at[s], recv_sem=recv_sem.at[s],
                device_id=(ix + dx, iy + dy), device_id_type=MESH,
            )
            for a, b, s in out
        ]

    def plane(i, j, block):
        a, f = SENT[i]
        row = block * 8 + (FRONT, PAD, PAD)[a]
        return (ve, ss, par)[a][f, j, row : row + 8, :]

    prepare_chunk(0)
    prepare_chunk(chunks - 1)
    for g in range(PAIRS):
        i0, i1 = 2 * g, min(2 * g + 1, NF - 1)
        for j in range(n):
            pack_u[g, j] = select(sub < 4, plane(i0, j, 0), roll(plane(i1, j, 0), 4, 0))
            pack_d[g, j] = select(sub < 4, roll(plane(i0, j, blocks - 1), 4, 0), plane(i1, j, blocks - 1))
    pl.semaphore_wait(barrier, count - 1)
    for d in DIRS[:2]:
        @pl.when(exists(d))
        def _():
            message(d, 0)[0].start()

    for c in range(1, chunks - 1):
        prepare_chunk(c)

    for i in range(2):
        for t in range(tall):
            x = packed[i, t * LANE : (t + 1) * LANE, :].T
            for f in range(8 * i, min(8 * i + 8, NF)):
                o = 16 * (f - 8 * i)
                own_r[f, t] = x[o : o + 8]
                own_l[f, t] = x[o + 8 : o + 16]
                a, g = SENT[f]
                dst = (col_va, col_sa, col_p)[a]
                dst[0, g, t, 16:24, :] = x[o + 8 : o + 16]
                dst[1, g, t, 8:16, :] = x[o : o + 8]
    up, down = zero, zero
    for i in range(2 * NF):
        src = own_l if i < NF else own_r
        g = (lane >= 4 * i) & (lane < 4 * i + 4)
        up = select(g, roll(src[i % NF, 0], 4 * i, 1), up)
        down = select(g, roll(src[i % NF, tall - 1], 4 * i + 4, 1), down)
    corner_u[...] = up
    corner_d[...] = down
    for d in DIRS[2:4]:
        @pl.when(exists(d))
        def _():
            message(d, 0)[0].start()
    for d in CORNERS:
        @pl.when(exists(d))
        def _():
            message(d, 1)[0].start()

    for i in range(NF):
        a, f = SENT[i]
        dst = (row_va, row_sa, row_p)[a]
        for j in range(n):
            x, y = (roll(plane(i, j, b), 4, 0) for b in (0, 1))
            dst[0, f, j, 8:16, :] = x
            dst[0, f, j, 16:24, :] = select(sub < 4, x, y)
            x, y = (roll(plane(i, j, b), 4, 0) for b in (blocks - 2, blocks - 1))
            dst[1, f, j, 8:16, :] = select(sub < 4, x, y)
            dst[1, f, j, 16:24, :] = y

    Stream(sw, ve, vx, ss, frc, par, rows).run()

    def clear(ref, lead):
        for i in lead:
            ref[i] = jnp.zeros(ref.shape[1:], f32)

    for d, buf in (((-1, 0), recv_u), ((1, 0), recv_d), ((0, -1), recv_l), ((0, 1), recv_r)):
        @pl.when(~exists(d))
        def _():
            clear(buf, range(buf.shape[0]))

    for c, d in enumerate(CORNERS):
        @pl.when(~exists(d))
        def _():
            corner_in[c] = zero

    for d in DIRS:
        @pl.when(exists(d))
        def _():
            for cp in message((-d[0], -d[1]), 2):
                cp.wait_recv()
            for cp in message(d, 2):
                cp.wait_send()

    for i in range(NF):
        a, f = SENT[i]
        dst = (row_va, row_sa, row_p)[a]
        g, odd = divmod(i, 2)
        for j in range(n):
            x, y = recv_u[g, j], recv_d[g, j]
            x = roll(x, 4, 0) if odd else x
            y = y if odd else roll(y, 4, 0)
            dst[0, f, j, 8:16, :] = select(sub < 4, x, dst[0, f, j, 8:16, :])
            dst[1, f, j, 16:24, :] = select(sub < 4, dst[1, f, j, 16:24, :], y)
        dst = (col_va, col_sa, col_p)[a]
        for t in range(tall):
            dst[0, f, t, 8:16, :] = recv_l[i, t]
            dst[1, f, t, 16:24, :] = recv_r[i, t]

        def corner(u, d, at):
            x = roll(corner_in[CORNERS.index(u)], LANE - 4 - 4 * at, 1)
            y = roll(corner_in[CORNERS.index(d)], -4 * at, 1)
            return select(lane < 4, y, select(lane >= LANE - 4, x, zero))

        dst[0, f, tall, 8:16, :] = corner((-1, -1), (1, -1), NF + i)
        dst[0, f, tall, 16:24, :] = corner((-1, 0), (1, 0), i)
        dst[1, f, tall, 8:16, :] = corner((-1, 0), (1, 0), NF + i)
        dst[1, f, tall, 16:24, :] = corner((-1, 1), (1, 1), i)

    strips = []
    for s, va, vb, sa, sb, x, fr, p in (
        (sw, row_va, row_vb, row_sa, row_sb, row_x, row_f, row_p),
        (Sweep(tall + 1, True), col_va, col_vb, col_sa, col_sb, col_x, col_f, col_p),
    ):
        for i in range(2):
            strips.append((s, i, *(View(y.at[i]) for y in (va, vb, sa, sb, x, fr, p))))

    def strip_cycles(t, carry):
        for flip in (False, True):
            for s, i, va, vb, sa, sb, x, fr, p in strips:
                for k in range(2):
                    s.spread(vb if flip else va, x, k)
            for s, i, va, vb, sa, sb, x, fr, p in strips:
                for k in range(2):
                    s.stress(vb if flip else va, x, *((sb, sa) if flip else (sa, sb)), p, k)
            for s, i, va, vb, sa, sb, x, fr, p in strips:
                for k in range(2):
                    s.force(sa if flip else sb, fr, k)
            for s, i, va, vb, sa, sb, x, fr, p in strips:
                for k in range(2):
                    s.velocity(*((vb, va, sa) if flip else (va, vb, sb)), fr, p, k)
        return carry

    lax.fori_loop(0, ITERS // 2, strip_cycles, 0)
    row_e, col_e = (row_va, row_sa), (col_va, col_sa)
    sums = [[zero, zero] for _ in range(n)]
    more = [zero, zero]
    for s, i, va, vb, sa, sb, x, fr, p in strips:
        for k in range(2):
            def add(j, x, y):
                if s.turned and (j == tall or k == i):
                    return
                good = sub >= 4 if k == 0 else sub < 4
                box = more if s.turned else sums[j]
                box[0] += select(good, x, zero)
                box[1] += select(good, y, zero)

            s.reduce(vb, va, p, k, add)

    last = FRONT + ITERS * rows
    acc[...] = jnp.zeros_like(acc)

    def reduce_rows(p, group, lead):
        part = {}

        def add(j, x, y):
            for i, z in ((2 * j, x), (2 * j + 1, y)):
                part[i] = part[i] + z if i in part else z

        base = pl.multiple_of(p * (8 * group), 8 * group)
        for i in range(group):
            sw.reduce(View(ve, last - rows + lead, base), View(ve, last + lead, base), View(par, PAD + lead, base), i, add)
        for i, z in part.items():
            acc[i] += z

    group = 2
    lax.fori_loop(0, (blocks - 2) // group, lambda p, c: (reduce_rows(p, group, 8), c)[1], 0)

    for j in range(n):
        good = lane >= 4 if j == 0 else lane < LANE - 4 if j == n - 1 else None
        if n == 1:
            good = (lane >= 4) & (lane < LANE - 4)
        for i in range(2):
            x = acc[2 * j + i] + sums[j][i]
            more[i] += x if good is None else jnp.where(good, x, 0.0)
    x, y = (jnp.sum(m, axis=0, keepdims=True) for m in more)
    x, y = x + roll(x, LANE // 2, 1), y + roll(y, LANE // 2, 1)
    half = lax.broadcasted_iota(jnp.int32, (1, LANE), 1) < LANE // 2
    part = jnp.where(half, x, y)
    mine[...] = part

    def sum_copy(k):
        return pltpu.make_async_remote_copy(
            src_ref=mine, dst_ref=slots.at[me], send_sem=sum_send.at[k], recv_sem=sum_recv.at[k],
            device_id=target(k), device_id_type=MESH,
        )

    def start(k, c):
        sum_copy(k).start()
        return c

    lax.fori_loop(1, count, start, 0)
    slots[pl.ds(me, 1)] = part[None]

    for t in range(tall):
        for o, (a, f) in enumerate(SENT[:5]):
            x = select(sub < 4, col_e[a][0, f, t, 16:24, :], col_e[a][1, f, t, 8:16, :])
            edge_t[o * 8 : o * 8 + 8, :] = roll(x, 4, 0)
        edge[t * LANE : (t + 1) * LANE, :] = edge_t[...].T

    def emit(rowsl, src):
        ev = edge[rowsl, :]
        es = [roll(ev, LANE - 4 - 8 * o, 1) for o in range(5)]
        for j in range(n):
            vals = [src[a][0][f, j, src[a][1], :] for a, f in SENT[:5]]
            if j == 0:
                vals = [select(lane < 4, e, x) for e, x in zip(es, vals)]
            if j == n - 1:
                vals = [select(lane >= LANE - 4, e, x) for e, x in zip(es, vals)]
            q, r, al, be, s2 = vals
            c = slice(j * LANE, (j + 1) * LANE)
            vel_out[0, rowsl, c] = 0.5 * (q + r)
            vel_out[1, rowsl, c] = 0.5 * (q - r)
            stress_out[0, rowsl, c] = 0.5 * (al + be)
            stress_out[1, rowsl, c] = s2
            stress_out[2, rowsl, c] = 0.25 * (al - be)

    def row_strip(i):
        return [(x.at[i], slice(12, 20)) for x in row_e]

    emit(slice(0, 8), row_strip(0))
    emit(slice(rows - 8, rows), row_strip(1))
    batch = 6 if (blocks - 2) % 6 == 0 else 2

    def body(p, c):
        base = pl.multiple_of(p * (8 * batch), 8)
        for i in range(1, batch + 1):
            src = [(ve, rows8((base, 8 * i + last))), (ss, rows8((base, 8 * i + PAD)))]
            emit(rows8((base, 8 * i)), src)
        return c

    lax.fori_loop(0, (blocks - 2) // batch, body, 0)

    def wait(k, c):
        sum_copy(k).wait()
        return c

    lax.fori_loop(1, count, wait, 0)
    total = slots[0]
    for i in range(1, count):
        total = total + slots[i]
    scale = 1.0 / (rows * nx * cols * ny)
    x = jnp.sum(jnp.where(half, total, 0.0), axis=1, keepdims=True) * (0.5 * scale)
    y = jnp.sum(jnp.where(half, 0.0, total), axis=1, keepdims=True) * (0.0625 * scale)
    total_out[...] = jnp.where(half, x, y)


def write_kernel(vel, stress, new_vel, new_stress, sem):
    copies = [
        pltpu.make_async_copy(vel, new_vel, sem.at[0]),
        pltpu.make_async_copy(stress, new_stress, sem.at[1]),
    ]
    for c in copies:
        c.start()
    for c in copies:
        c.wait()


def per_device(nx, ny, velocity, stress, strength, ice_mass, wind, current, ice_mask, open_water):
    _, rows, cols = velocity.shape
    n, tall, strip = cols // LANE, rows // LANE, rows + 2 * PAD
    i32 = jnp.int32
    vmem = pl.BlockSpec(memory_space=pltpu.VMEM)
    hbm = pl.BlockSpec(memory_space=pl.ANY)
    dma = pltpu.SemaphoreType.DMA
    V = pltpu.VMEM
    count = nx * ny
    new_vel, new_stress, total = pl.pallas_call(
        functools.partial(core_kernel, nx, ny, rows, cols),
        out_shape=(V((2, rows, cols), f32), V((3, rows, cols), f32), V((1, LANE), f32)),
        in_specs=[pl.BlockSpec(memory_space=pltpu.HBM)] * 8,
        out_specs=(vmem, vmem, vmem),
        scratch_shapes=[
            V((rows, cols), f32), V((rows, cols), f32), V((rows, cols), i32), V((rows, cols), i32),
            V((2, rows, cols), f32), V((3, rows, cols), f32), V((2, rows, cols), f32), V((2, rows, cols), f32),
            V((2, n, FRONT + (ITERS + 1) * rows, LANE), f32), V((2, n, 2 * rows + PAD, LANE), f32),
            V((3, n, strip, LANE), f32), V((2, n, 2 * 8 * UN + PAD, LANE), f32),
            V((6, n, strip, LANE), f32), V((2 * n, 8, LANE), f32),
            V((PAIRS, n, 8, LANE), f32), V((PAIRS, n, 8, LANE), f32),
            V((PAIRS, n, 8, LANE), f32), V((PAIRS, n, 8, LANE), f32),
            V((NF, tall, 8, LANE), f32), V((NF, tall, 8, LANE), f32),
            V((NF, tall, 8, LANE), f32), V((NF, tall, 8, LANE), f32),
            V((8, LANE), f32), V((8, LANE), f32), V((6, 8, LANE), f32),
            V((2, 2, n, 32, LANE), f32), V((2, 2, n, 32, LANE), f32),
            V((2, 3, n, 32, LANE), f32), V((2, 3, n, 32, LANE), f32), V((2, 2, n, 32, LANE), f32),
            V((2, 2, n, 32, LANE), f32), V((2, 6, n, 32, LANE), f32),
            V((2, 2, tall + 1, 32, LANE), f32), V((2, 2, tall + 1, 32, LANE), f32),
            V((2, 3, tall + 1, 32, LANE), f32), V((2, 3, tall + 1, 32, LANE), f32), V((2, 2, tall + 1, 32, LANE), f32),
            V((2, 2, tall + 1, 32, LANE), f32), V((2, 6, tall + 1, 32, LANE), f32),
            V((2, rows, LANE), f32), V((LANE, LANE), f32), V((rows, LANE), f32),
            V((1, LANE), f32), V((count, 1, LANE), f32),
            dma((8, 8)), dma((10,)), dma((10,)), dma((count,)), dma((count,)),
        ],
        compiler_params=pltpu.CompilerParams(
            collective_id=0, has_side_effects=True, vmem_limit_bytes=48 << 20
        ),
        name="core",
    )(
        *[
            pltpu.with_memory_space_constraint(x, pltpu.HBM)
            for x in (velocity, stress, strength, ice_mass, wind, current, ice_mask, open_water)
        ]
    )
    new_vel, new_stress = pl.pallas_call(
        write_kernel,
        out_shape=(
            jax.ShapeDtypeStruct(velocity.shape, f32),
            jax.ShapeDtypeStruct(stress.shape, f32),
        ),
        in_specs=[vmem, vmem],
        out_specs=(hbm, hbm),
        scratch_shapes=[dma((2,))],
        compiler_params=pltpu.CompilerParams(vmem_limit_bytes=8 << 20),
        name="write",
    )(new_vel, new_stress)
    return new_vel, new_stress, total[0, 0], total[0, LANE - 1]


def solution(mesh):
    two, three = P("gx", "gy"), P(None, "gx", "gy")
    return jax.shard_map(
        functools.partial(per_device, mesh.shape["gx"], mesh.shape["gy"]),
        mesh=mesh,
        in_specs=(three, three, two, two, three, three, two, two),
        out_specs=(three, three, P(), P()),
        check_vma=False,
    )
```

```python
import functools

import jax
import jax.numpy as jnp
from jax import lax
from jax.experimental import pallas as pl
from jax.experimental.pallas import tpu as pltpu
from jax.sharding import PartitionSpec as P

ITERS = 4
relax_rate = 0.8
time_step = 0.5
drag_coef = 1.0
coriolis = 0.3
delta_floor = 0.05
MESH = pl.DeviceIdType.MESH

Q, R = range(2)
AL, S2, BE = range(3)
PR, M, TQ, TR, CA, CB = range(6)
SENT = ((0, Q), (0, R), (1, AL), (1, BE), (1, S2)) + tuple((2, f) for f in range(6))
NF = len(SENT)
PAIRS = (NF + 1) // 2
LANE = 128
PAD = 8
FRONT = 128
UN = 4
DIRS = ((-1, 0), (1, 0), (0, -1), (0, 1), (-1, -1), (-1, 1), (1, -1), (1, 1))
CORNERS = ((-1, 0), (1, 0)) + DIRS[4:]
f32 = jnp.float32


def iota(axis):
    return lax.broadcasted_iota(jnp.int32, (8, LANE), axis)


def roll(x, by, axis):
    by %= x.shape[axis]
    return pltpu.roll(x, by, axis=axis) if by else x


def rows8(row):
    if isinstance(row, int):
        return slice(row, row + 8)
    base, off = row
    return pl.ds(base + off if off % 8 else pl.multiple_of(base + off, 8), 8)


def select(mask, x, y):
    return lax.select(mask, x, y)


def shift(xs, by, first, last):
    n = len(xs)
    turned = [roll(x, by, 1) for x in xs]
    if by > 0:
        return [select(first, turned[(j - 1) % n], turned[j]) for j in range(n)]
    return [select(last, turned[(j + 1) % n], turned[j]) for j in range(n)]


class View:
    def __init__(self, ref, pad=PAD, base=None):
        self.ref, self.pad, self.base = ref, pad, base

    def at(self, i, off=0):
        row = self.pad + 8 * i + off
        return rows8(row if self.base is None else (self.base, row))

    def load(self, f, j, i, off=0):
        return self.ref[f, j, self.at(i, off), :]

    def store(self, f, j, i, x):
        self.ref[f, j, self.at(i), :] = x


class Sweep:
    def __init__(self, tiles, turned):
        self.n, self.turned = tiles, turned
        self.first, self.last = iota(1) == 0, iota(1) == LANE - 1

    def spread(self, ve, vx, i):
        for f in (Q, R):
            xs = shift([ve.load(f, j, i) for j in range(self.n)], 1, self.first, self.last)
            for j, x in enumerate(xs):
                vx.store(f, j, i, x)

    def stress(self, ve, vx, old, new, par, i):
        keep = 1.0 / (1.0 + relax_rate)
        for j in range(self.n):
            q, r, qx, rx = (v.load(f, j, i) for v in (ve, vx) for f in (Q, R))
            qa, ra, qxa, rxa = (v.load(f, j, i, -1) for v in (ve, vx) for f in (Q, R))
            a, b = q - qxa, rx - ra
            if self.turned:
                d, s = a - b, a + b
                t = (r - rxa) - (qx - qa)
            else:
                d, s = a + b, a - b
                t = (r - rxa) + (qx - qa)
            e = (d * d + 4.0 * delta_floor * delta_floor) + 0.25 * (t * t + s * s)
            pr = par.load(PR, j, i)
            g = pr * lax.rsqrt(e)
            h = 0.25 * g
            push, side = g * d - pr, h * s
            new.store(AL, j, i, old.load(AL, j, i) * keep + (push + side))
            new.store(BE, j, i, old.load(BE, j, i) * keep + (push - side))
            new.store(S2, j, i, old.load(S2, j, i) * keep + h * t)

    def force(self, ss, frc, i):
        a, c = [], []
        for j in range(self.n):
            ad, s, sd, b = ss.load(AL, j, i, 1), ss.load(S2, j, i), ss.load(S2, j, i, 1), ss.load(BE, j, i)
            if self.turned:
                a.append(ad + s)
                c.append(sd + b)
            else:
                a.append(ad - s)
                c.append(sd - b)
        for f, xs in ((0, a), (1, c)):
            for j, x in enumerate(shift(xs, -1, self.first, self.last)):
                frc.store(f, j, i, x)

    def velocity(self, old, new, ss, frc, par, i):
        for j in range(self.n):
            al, s, sd, bd = ss.load(AL, j, i), ss.load(S2, j, i), ss.load(S2, j, i, 1), ss.load(BE, j, i, 1)
            fa, fc = frc.load(0, j, i), frc.load(1, j, i)
            if self.turned:
                fq, fr = fa - (sd + al), fc - (bd + s)
            else:
                fq, fr = fa + (sd - al), fc + (bd - s)
            q, r, m = old.load(Q, j, i), old.load(R, j, i), par.load(M, j, i)
            x = m * q + (fq + par.load(TQ, j, i))
            y = m * r + (fr + par.load(TR, j, i))
            ca, cb = par.load(CA, j, i), par.load(CB, j, i)
            new.store(Q, j, i, ca * x - cb * y)
            new.store(R, j, i, ca * y + cb * x)

    def reduce(self, old, new, par, i, add):
        for j in range(self.n):
            nq, nr = new.load(Q, j, i), new.load(R, j, i)
            dq, dr = nq - old.load(Q, j, i), nr - old.load(R, j, i)
            add(j, dq * dq + dr * dr, par.load(M, j, i) * (nq * nq + nr * nr))


class Stream:
    def __init__(self, sw, ve, vx, ss, frc, par, rows):
        self.sw, self.ve, self.vx, self.ss, self.frc, self.par, self.rows = sw, ve, vx, ss, frc, par, rows

    def step(self, p, stages):
        sw, rows, unit = self.sw, self.rows, 8 * UN
        row = pl.multiple_of(p * unit, unit)
        turn = pl.multiple_of(lax.rem(row, rows), unit)
        late = pl.multiple_of(lax.rem(row + rows - 4 * unit, rows), unit)
        slots = [View(self.frc, PAD, pl.multiple_of(lax.rem(p + k, 2) * unit, unit)) for k in (0, 1)]
        was = lambda ref, lag: View(ref, FRONT - lag * unit, row)
        now = lambda ref, lag: View(ref, FRONT + rows - lag * unit, row)
        par = lambda lag: View(self.par, FRONT - lag * unit, turn)
        ve, ss = self.ve, self.ss
        todo = {
            "velocity": (was(ve, 3), now(ve, 3), now(ss, 3), slots[1], par(3)),
            "force": (now(ss, 2), slots[0]),
            "stress": (was(ve, 0), View(self.vx, PAD, turn), was(ss, 0), now(ss, 0), par(0)),
            "spread": (now(ve, 4), View(self.vx, PAD, late)),
        }
        for name in stages:
            for i in range(UN):
                getattr(sw, name)(*todo[name], i)

    def run(self, lo, hi):
        every = ("velocity", "force", "stress", "spread")
        steps = ITERS * self.rows // (8 * UN)
        for a, b, stages in (
            (0, 2, every[2:3]), (2, 3, every[1:3]), (3, 4, every[:3]),
            (4, steps, every), (steps, steps + 2, every[:2]), (steps + 2, steps + 3, every[:1]),
        ):
            if isinstance(lo, int):
                a, b = max(a, lo), min(b, hi)
                if a >= b:
                    continue
            elif a != 4:
                continue
            else:
                a, b = lo, hi

            def body(p, carry):
                self.step(p, stages)
                return carry

            lax.fori_loop(a, b, body, 0)


def core_kernel(
    nx, ny, rows, cols,
    vel, stress, strength, mass, wind, current, mask, water,
    vel_out, stress_out, total_out,
    strength_v, mass_v, mask_v, water_v, wind_v, current_v,
    ve, vx, ss, frc, par, acc,
    pack_u, pack_d, recv_u, recv_d, own_l, own_r, recv_l, recv_r,
    corner_u, corner_d, corner_in,
    row_va, row_vb, row_sa, row_sb, row_x, row_f, row_p, col_va, col_vb, col_sa, col_sb, col_x, col_f, col_p,
    packed, edge_t, edge, mine, slots,
    load_sem, send_sem, recv_sem, sum_send, sum_recv,
):
    ix = lax.axis_index("gx")
    iy = lax.axis_index("gy")
    n, tall, blocks = cols // LANE, rows // LANE, rows // 8
    chunks = 8
    per = rows // chunks
    lane, sub = iota(1), iota(0)
    zero = jnp.zeros((8, LANE), f32)

    def loads(c):
        part = pl.ds(pl.multiple_of(c * per, 8), per)
        later = pl.ds(pl.multiple_of(c * per + FRONT, 8), per)
        both = slice(None)
        pairs = [
            (strength.at[part], strength_v.at[part]),
            (mass.at[part], mass_v.at[part]),
            (mask.at[part], mask_v.at[part]),
            (water.at[part], water_v.at[part]),
            (wind.at[both, part], wind_v.at[both, part]),
            (current.at[both, part], current_v.at[both, part]),
        ]
        for j in range(n):
            tile = pl.ds(j * LANE, LANE)
            pairs.append((vel.at[both, part, tile], ve.at[both, j, later]))
            pairs.append((stress.at[both, part, tile], ss.at[both, j, later]))
        return [pltpu.make_async_copy(a, b, load_sem.at[c, k]) for k, (a, b) in enumerate(pairs)]

    for c in [0, chunks - 1] + list(range(1, chunks - 1)):
        for cp in loads(c):
            cp.start()

    count = nx * ny
    me = ix * ny + iy

    def others(act):
        def line(x, carry):
            for y in range(ny):
                @pl.when((x != ix) | (y != iy))
                def _():
                    act(x, y)
            return carry

        lax.fori_loop(0, nx, line, 0)

    barrier = pltpu.get_barrier_semaphore()
    others(lambda x, y: pl.semaphore_signal(barrier, inc=1, device_id=(x, y), device_id_type=MESH))

    for j in range(n):
        for f in range(2):
            ve[f, j, FRONT - 8 : FRONT, :] = zero
            vx[f, j, 0:8, :] = zero
        for f in range(3):
            ss[f, j, FRONT + (ITERS + 1) * rows : FRONT + (ITERS + 1) * rows + 8, :] = zero
    for st in (row_va, row_vb, row_sa, row_sb, row_x, col_va, col_vb, col_sa, col_sb, col_x):
        for side in range(2):
            for f in range(st.shape[1]):
                for j in range(st.shape[2]):
                    st[side, f, j, 0:8, :] = zero
                    st[side, f, j, 24:32, :] = zero

    sw = Sweep(n, False)

    def prepare(base, i):
        rowsl, at = rows8((base, 8 * i)), rows8((base, 8 * i + FRONT))
        ends = []
        for j in range(n):
            src = (rowsl, slice(j * LANE, (j + 1) * LANE))
            w = mask_v[src].astype(f32) * (1.0 - water_v[src].astype(f32))
            m = mass_v[src]
            inertia = m * (1.0 / time_step)
            diagonal = inertia + drag_coef
            turning = m * coriolis
            scale = (0.5 * w) / (diagonal * diagonal + turning * turning)
            tx = wind_v[(0,) + src] + drag_coef * current_v[(0,) + src]
            ty = wind_v[(1,) + src] + drag_coef * current_v[(1,) + src]
            u, v = ve[0, j, at, :], ve[1, j, at, :]
            s1, s2, s12 = (ss[f, j, at, :] for f in range(3))
            t = s12 + s12
            q, r = u + v, u - v
            moving = {Q: q, R: r}
            state = {AL: s1 + t, BE: s1 - t, S2: s2}
            fixed = {
                PR: strength_v[src] * w * (relax_rate / (1.0 + relax_rate)),
                M: inertia * 2.0,
                TQ: (tx + ty) * 2.0,
                TR: (tx - ty) * 2.0,
                CA: diagonal * scale,
                CB: turning * scale,
            }
            for f, x in moving.items():
                ve[f, j, at, :] = x
            for f, x in ((AL, state[AL]), (BE, state[BE])):
                ss[f, j, at, :] = x
            for f, x in fixed.items():
                par[f, j, at, :] = x
            if j in (0, n - 1):
                ends.append([(moving, state, fixed)[a][f] for a, f in SENT])
        low, high = ends[0], ends[-1]
        packs = [zero, zero]
        for i in range(NF):
            x = roll(select(lane < LANE // 2, low[i], high[i]), 16 * (i % 8) + 8, 1)
            g = (lane >= 16 * (i % 8)) & (lane < 16 * (i % 8) + 16)
            packs[i // 8] = select(g, x, packs[i // 8])
        for i in range(2):
            packed[i, rowsl, :] = packs[i]

    group = min(UN, per // 8)

    def prepare_chunk(c):
        for cp in loads(c):
            cp.wait()

        def body(p, carry):
            base = pl.multiple_of(c * per + p * (8 * group), 8 * group)
            for i in range(group):
                prepare(base, i)
            for i in range(group):
                sw.spread(View(ve, FRONT, base), View(vx, PAD, base), i)
            return carry

        lax.fori_loop(0, per // 8 // group, body, 0)

    def exists(d):
        return (ix + d[0] >= 0) & (ix + d[0] < nx) & (iy + d[1] >= 0) & (iy + d[1] < ny)

    def message(d, which):
        k = DIRS.index(d)
        dx, dy = d
        out = []
        if which == 1:
            pass
        elif dy == 0:
            out.append((pack_u, recv_d, k) if dx < 0 else (pack_d, recv_u, k))
        elif dx == 0:
            out.append((own_l, recv_r, k) if dy < 0 else (own_r, recv_l, k))
        if dx and which != 0:
            c = CORNERS.index(d)
            back = CORNERS.index((-dx, -dy))
            out.append((corner_u if dx < 0 else corner_d, corner_in.at[back], 4 + c))
        return [
            pltpu.make_async_remote_copy(
                src_ref=a, dst_ref=b, send_sem=send_sem.at[s], recv_sem=recv_sem.at[s],
                device_id=(ix + dx, iy + dy), device_id_type=MESH,
            )
            for a, b, s in out
        ]

    def plane(i, j, block):
        a, f = SENT[i]
        row = block * 8 + FRONT
        return (ve, ss, par)[a][f, j, row : row + 8, :]

    prepare_chunk(0)
    prepare_chunk(chunks - 1)
    for g in range(PAIRS):
        i0, i1 = 2 * g, min(2 * g + 1, NF - 1)
        for j in range(n):
            pack_u[g, j] = select(sub < 4, plane(i0, j, 0), roll(plane(i1, j, 0), 4, 0))
            pack_d[g, j] = select(sub < 4, roll(plane(i0, j, blocks - 1), 4, 0), plane(i1, j, blocks - 1))
    pl.semaphore_wait(barrier, count - 1)
    for d in DIRS[:2]:
        @pl.when(exists(d))
        def _():
            message(d, 0)[0].start()

    for i in range(NF):
        a, f = SENT[i]
        dst = (row_va, row_sa, row_p)[a]
        for j in range(n):
            x, y = (roll(plane(i, j, b), 4, 0) for b in (0, 1))
            dst[0, f, j, 8:16, :] = x
            dst[0, f, j, 16:24, :] = select(sub < 4, x, y)
            x, y = (roll(plane(i, j, b), 4, 0) for b in (blocks - 2, blocks - 1))
            dst[1, f, j, 8:16, :] = select(sub < 4, x, y)
            dst[1, f, j, 16:24, :] = y

    stream = Stream(sw, ve, vx, ss, frc, par, rows)
    pace = per // (8 * UN)
    begin = 1
    if pace:
        stream.run(0, pace)
        while begin < chunks - 1 and begin * pace < 4:
            prepare_chunk(begin)
            stream.run(begin * pace, (begin + 1) * pace)
            begin += 1

    def advance(c, carry):
        prepare_chunk(c)
        if pace:
            stream.run(c * pace, (c + 1) * pace)
        return carry

    lax.fori_loop(begin, chunks - 1, advance, 0)

    def wrap(i, carry):
        for f in range(6):
            for j in range(n):
                par[f, j, rows8((8 * i, FRONT - 24 * UN)), :] = par[f, j, rows8((8 * i, FRONT + rows - 24 * UN)), :]
        return carry

    lax.fori_loop(0, 3 * UN, wrap, 0)

    for i in range(2):
        for t in range(tall):
            x = packed[i, t * LANE : (t + 1) * LANE, :].T
            for f in range(8 * i, min(8 * i + 8, NF)):
                o = 16 * (f - 8 * i)
                own_r[f, t] = x[o : o + 8]
                own_l[f, t] = x[o + 8 : o + 16]
                a, g = SENT[f]
                dst = (col_va, col_sa, col_p)[a]
                dst[0, g, t, 16:24, :] = x[o + 8 : o + 16]
                dst[1, g, t, 8:16, :] = x[o : o + 8]
    up, down = zero, zero
    for i in range(2 * NF):
        src = own_l if i < NF else own_r
        g = (lane >= 4 * i) & (lane < 4 * i + 4)
        up = select(g, roll(src[i % NF, 0], 4 * i, 1), up)
        down = select(g, roll(src[i % NF, tall - 1], 4 * i + 4, 1), down)
    corner_u[...] = up
    corner_d[...] = down
    for d in DIRS[2:4]:
        @pl.when(exists(d))
        def _():
            message(d, 0)[0].start()
    for d in CORNERS:
        @pl.when(exists(d))
        def _():
            message(d, 1)[0].start()

    stream.run((chunks - 1) * pace, ITERS * blocks // UN + 3)

    def clear(ref, lead):
        for i in lead:
            ref[i] = jnp.zeros(ref.shape[1:], f32)

    for d, buf in (((-1, 0), recv_u), ((1, 0), recv_d), ((0, -1), recv_l), ((0, 1), recv_r)):
        @pl.when(~exists(d))
        def _():
            clear(buf, range(buf.shape[0]))

    for c, d in enumerate(CORNERS):
        @pl.when(~exists(d))
        def _():
            corner_in[c] = zero

    for d in DIRS:
        @pl.when(exists(d))
        def _():
            for cp in message((-d[0], -d[1]), 2):
                cp.wait_recv()
            for cp in message(d, 2):
                cp.wait_send()

    for i in range(NF):
        a, f = SENT[i]
        dst = (row_va, row_sa, row_p)[a]
        g, odd = divmod(i, 2)
        for j in range(n):
            x, y = recv_u[g, j], recv_d[g, j]
            x = roll(x, 4, 0) if odd else x
            y = y if odd else roll(y, 4, 0)
            dst[0, f, j, 8:16, :] = select(sub < 4, x, dst[0, f, j, 8:16, :])
            dst[1, f, j, 16:24, :] = select(sub < 4, dst[1, f, j, 16:24, :], y)
        dst = (col_va, col_sa, col_p)[a]
        for t in range(tall):
            dst[0, f, t, 8:16, :] = recv_l[i, t]
            dst[1, f, t, 16:24, :] = recv_r[i, t]

        def corner(u, d, at):
            x = roll(corner_in[CORNERS.index(u)], LANE - 4 - 4 * at, 1)
            y = roll(corner_in[CORNERS.index(d)], -4 * at, 1)
            return select(lane < 4, y, select(lane >= LANE - 4, x, zero))

        dst[0, f, tall, 8:16, :] = corner((-1, -1), (1, -1), NF + i)
        dst[0, f, tall, 16:24, :] = corner((-1, 0), (1, 0), i)
        dst[1, f, tall, 8:16, :] = corner((-1, 0), (1, 0), NF + i)
        dst[1, f, tall, 16:24, :] = corner((-1, 1), (1, 1), i)

    strips = []
    for s, va, vb, sa, sb, x, fr, p in (
        (sw, row_va, row_vb, row_sa, row_sb, row_x, row_f, row_p),
        (Sweep(tall + 1, True), col_va, col_vb, col_sa, col_sb, col_x, col_f, col_p),
    ):
        for i in range(2):
            strips.append((s, i, *(View(y.at[i]) for y in (va, vb, sa, sb, x, fr, p))))

    def strip_cycles(t, carry):
        for flip in (False, True):
            for s, i, va, vb, sa, sb, x, fr, p in strips:
                for k in range(2):
                    s.spread(vb if flip else va, x, k)
            for s, i, va, vb, sa, sb, x, fr, p in strips:
                for k in range(2):
                    s.stress(vb if flip else va, x, *((sb, sa) if flip else (sa, sb)), p, k)
            for s, i, va, vb, sa, sb, x, fr, p in strips:
                for k in range(2):
                    s.force(sa if flip else sb, fr, k)
            for s, i, va, vb, sa, sb, x, fr, p in strips:
                for k in range(2):
                    s.velocity(*((vb, va, sa) if flip else (va, vb, sb)), fr, p, k)
        return carry

    lax.fori_loop(0, ITERS // 2, strip_cycles, 0)
    row_e, col_e = (row_va, row_sa), (col_va, col_sa)
    sums = [[zero, zero] for _ in range(n)]
    more = [zero, zero]
    for s, i, va, vb, sa, sb, x, fr, p in strips:
        for k in range(2):
            def add(j, x, y):
                if s.turned and (j == tall or k == i):
                    return
                good = sub >= 4 if k == 0 else sub < 4
                box = more if s.turned else sums[j]
                box[0] += select(good, x, zero)
                box[1] += select(good, y, zero)

            s.reduce(vb, va, p, k, add)

    last = FRONT + ITERS * rows
    acc[...] = jnp.zeros_like(acc)

    def reduce_rows(p, group, lead):
        part = {}

        def add(j, x, y):
            for i, z in ((2 * j, x), (2 * j + 1, y)):
                part[i] = part[i] + z if i in part else z

        base = pl.multiple_of(p * (8 * group), 8 * group)
        for i in range(group):
            sw.reduce(View(ve, last - rows + lead, base), View(ve, last + lead, base), View(par, FRONT + lead, base), i, add)
        for i, z in part.items():
            acc[i] += z

    lax.fori_loop(0, (blocks - 2) // 2, lambda p, c: (reduce_rows(p, 2, 8), c)[1], 0)

    for j in range(n):
        good = lane >= 4 if j == 0 else lane < LANE - 4 if j == n - 1 else None
        if n == 1:
            good = (lane >= 4) & (lane < LANE - 4)
        for i in range(2):
            x = acc[2 * j + i] + sums[j][i]
            more[i] += x if good is None else jnp.where(good, x, 0.0)
    x, y = (jnp.sum(m, axis=0, keepdims=True) for m in more)
    x, y = x + roll(x, LANE // 2, 1), y + roll(y, LANE // 2, 1)
    half = lax.broadcasted_iota(jnp.int32, (1, LANE), 1) < LANE // 2
    part = jnp.where(half, x, y)
    mine[...] = part

    def sum_copy(x, y, origin):
        return pltpu.make_async_remote_copy(
            src_ref=mine, dst_ref=slots.at[me], send_sem=sum_send.at[x * ny + y],
            recv_sem=sum_recv.at[origin], device_id=(x, y), device_id_type=MESH,
        )

    others(lambda x, y: sum_copy(x, y, me).start())
    slots[pl.ds(me, 1)] = part[None]

    for t in range(tall):
        for o, (a, f) in enumerate(SENT[:5]):
            x = select(sub < 4, col_e[a][0, f, t, 16:24, :], col_e[a][1, f, t, 8:16, :])
            edge_t[t, o * 8 : o * 8 + 8, :] = roll(x, 4, 0)
    for t in range(tall):
        edge[t * LANE : (t + 1) * LANE, :] = edge_t[t].T

    def emit(rowsl, src):
        ev = edge[rowsl, :]
        es = [roll(ev, LANE - 4 - 8 * o, 1) for o in range(5)]
        for j in range(n):
            vals = [src[a][0][f, j, src[a][1], :] for a, f in SENT[:5]]
            if j == 0:
                vals = [select(lane < 4, e, x) for e, x in zip(es, vals)]
            if j == n - 1:
                vals = [select(lane >= LANE - 4, e, x) for e, x in zip(es, vals)]
            q, r, al, be, s2 = vals
            c = slice(j * LANE, (j + 1) * LANE)
            vel_out[0, rowsl, c] = 0.5 * (q + r)
            vel_out[1, rowsl, c] = 0.5 * (q - r)
            stress_out[0, rowsl, c] = 0.5 * (al + be)
            stress_out[1, rowsl, c] = s2
            stress_out[2, rowsl, c] = 0.25 * (al - be)

    def row_strip(i):
        return [(x.at[i], slice(12, 20)) for x in row_e]

    emit(slice(0, 8), row_strip(0))
    emit(slice(rows - 8, rows), row_strip(1))

    def emit_rows(base, count):
        for i in range(1, count + 1):
            at = rows8((base, 8 * i + last))
            emit(rows8((base, 8 * i)), [(ve, at), (ss, at)])

    batch = min(10, blocks - 2)

    def body(p, c):
        emit_rows(pl.multiple_of(p * (8 * batch), 8), batch)
        return c

    lax.fori_loop(0, (blocks - 2) // batch, body, 0)
    emit_rows((blocks - 2) // batch * batch * 8, (blocks - 2) % batch)

    others(lambda x, y: sum_copy(x, y, x * ny + y).wait())
    total = slots[0]
    for i in range(1, count):
        total = total + slots[i]
    scale = 1.0 / (rows * nx * cols * ny)
    x = jnp.sum(jnp.where(half, total, 0.0), axis=1, keepdims=True) * (0.5 * scale)
    y = jnp.sum(jnp.where(half, 0.0, total), axis=1, keepdims=True) * (0.0625 * scale)
    total_out[...] = jnp.where(half, x, y)


def write_kernel(vel, stress, total, new_vel, new_stress, residual, kinetic, sem):
    copies = [
        pltpu.make_async_copy(a.at[f, part], b.at[f, part], sem.at[k, f, h])
        for k, (a, b) in enumerate(((vel, new_vel), (stress, new_stress)))
        for f in range(a.shape[0])
        for h, part in enumerate((pl.ds(0, a.shape[1] // 2), pl.ds(a.shape[1] // 2, a.shape[1] // 2)))
    ]
    for c in copies:
        c.start()
    x = total[...]
    residual[0, 0] = x[0, 0]
    kinetic[0, 0] = x[0, LANE - 1]
    for c in copies:
        c.wait()


def per_device(nx, ny, velocity, stress, strength, ice_mass, wind, current, ice_mask, open_water):
    _, rows, cols = velocity.shape
    n, tall, strip = cols // LANE, rows // LANE, rows + 2 * PAD
    i32 = jnp.int32
    vmem = pl.BlockSpec(memory_space=pltpu.VMEM)
    hbm = pl.BlockSpec(memory_space=pl.ANY)
    dma = pltpu.SemaphoreType.DMA
    V = pltpu.VMEM
    count = nx * ny
    new_vel, new_stress, total = pl.pallas_call(
        functools.partial(core_kernel, nx, ny, rows, cols),
        out_shape=(V((2, rows, cols), f32), V((3, rows, cols), f32), V((1, LANE), f32)),
        in_specs=[pl.BlockSpec(memory_space=pltpu.HBM)] * 8,
        out_specs=(vmem, vmem, vmem),
        scratch_shapes=[
            V((rows, cols), f32), V((rows, cols), f32), V((rows, cols), i32), V((rows, cols), i32),
            V((2, rows, cols), f32), V((2, rows, cols), f32),
            V((2, n, FRONT + (ITERS + 1) * rows, LANE), f32), V((2, n, rows + PAD, LANE), f32),
            V((3, n, FRONT + (ITERS + 1) * rows + 8, LANE), f32), V((2, n, 2 * 8 * UN + PAD, LANE), f32),
            V((6, n, FRONT + rows, LANE), f32), V((2 * n, 8, LANE), f32),
            V((PAIRS, n, 8, LANE), f32), V((PAIRS, n, 8, LANE), f32),
            V((PAIRS, n, 8, LANE), f32), V((PAIRS, n, 8, LANE), f32),
            V((NF, tall, 8, LANE), f32), V((NF, tall, 8, LANE), f32),
            V((NF, tall, 8, LANE), f32), V((NF, tall, 8, LANE), f32),
            V((8, LANE), f32), V((8, LANE), f32), V((6, 8, LANE), f32),
            V((2, 2, n, 32, LANE), f32), V((2, 2, n, 32, LANE), f32),
            V((2, 3, n, 32, LANE), f32), V((2, 3, n, 32, LANE), f32), V((2, 2, n, 32, LANE), f32),
            V((2, 2, n, 32, LANE), f32), V((2, 6, n, 32, LANE), f32),
            V((2, 2, tall + 1, 32, LANE), f32), V((2, 2, tall + 1, 32, LANE), f32),
            V((2, 3, tall + 1, 32, LANE), f32), V((2, 3, tall + 1, 32, LANE), f32), V((2, 2, tall + 1, 32, LANE), f32),
            V((2, 2, tall + 1, 32, LANE), f32), V((2, 6, tall + 1, 32, LANE), f32),
            V((2, rows, LANE), f32), V((tall, LANE, LANE), f32), V((rows, LANE), f32),
            V((1, LANE), f32), V((count, 1, LANE), f32),
            dma((8, 6 + 2 * n)), dma((10,)), dma((10,)), dma((count,)), dma((count,)),
        ],
        compiler_params=pltpu.CompilerParams(
            collective_id=0, has_side_effects=True, vmem_limit_bytes=57 << 20
        ),
        name="core",
    )(
        *[
            pltpu.with_memory_space_constraint(x, pltpu.HBM)
            for x in (velocity, stress, strength, ice_mass, wind, current, ice_mask, open_water)
        ]
    )
    smem = pl.BlockSpec(memory_space=pltpu.SMEM)
    new_vel, new_stress, residual, kinetic = pl.pallas_call(
        write_kernel,
        out_shape=(
            jax.ShapeDtypeStruct(velocity.shape, f32),
            jax.ShapeDtypeStruct(stress.shape, f32),
            jax.ShapeDtypeStruct((1, 1), f32),
            jax.ShapeDtypeStruct((1, 1), f32),
        ),
        in_specs=[vmem, vmem, vmem],
        out_specs=(hbm, hbm, smem, smem),
        scratch_shapes=[dma((2, 3, 2))],
        compiler_params=pltpu.CompilerParams(vmem_limit_bytes=1 << 20),
        name="write",
    )(new_vel, new_stress, total)
    return new_vel, new_stress, residual.reshape(()), kinetic.reshape(())


def solution(mesh):
    two, three = P("gx", "gy"), P(None, "gx", "gy")
    return jax.shard_map(
        functools.partial(per_device, mesh.shape["gx"], mesh.shape["gy"]),
        mesh=mesh,
        in_specs=(three, three, two, two, three, three, two, two),
        out_specs=(three, three, P(), P()),
        check_vma=False,
    )
```

```python
import functools

import jax
import jax.numpy as jnp
from jax import lax
from jax.experimental import pallas as pl
from jax.experimental.pallas import tpu as pltpu
from jax.sharding import PartitionSpec as P

ITERS = 4
relax_rate = 0.8
time_step = 0.5
drag_coef = 1.0
coriolis = 0.3
delta_floor = 0.05
MESH = pl.DeviceIdType.MESH

Q, R = range(2)
AL, S2, BE = range(3)
PR, M, TQ, TR, CA, CB = range(6)
SENT = ((0, Q), (0, R), (1, AL), (1, BE), (1, S2)) + tuple((2, f) for f in range(6))
NF = len(SENT)
PAIRS = (NF + 1) // 2
LANE = 128
PAD = 8
FRONT = 128
UN = 4
DIRS = ((-1, 0), (1, 0), (0, -1), (0, 1), (-1, -1), (-1, 1), (1, -1), (1, 1))
CORNERS = ((-1, 0), (1, 0)) + DIRS[4:]
f32 = jnp.float32


def iota(axis):
    return lax.broadcasted_iota(jnp.int32, (8, LANE), axis)


def roll(x, by, axis):
    by %= x.shape[axis]
    return pltpu.roll(x, by, axis=axis) if by else x


def rows8(row):
    if isinstance(row, int):
        return slice(row, row + 8)
    base, off = row
    return pl.ds(base + off if off % 8 else pl.multiple_of(base + off, 8), 8)


def select(mask, x, y):
    return lax.select(mask, x, y)


def shift(xs, by, first, last):
    n = len(xs)
    turned = [roll(x, by, 1) for x in xs]
    if by > 0:
        return [select(first, turned[(j - 1) % n], turned[j]) for j in range(n)]
    return [select(last, turned[(j + 1) % n], turned[j]) for j in range(n)]


class View:
    def __init__(self, ref, pad=PAD, base=None):
        self.ref, self.pad, self.base = ref, pad, base

    def at(self, i, off=0):
        row = self.pad + 8 * i + off
        return rows8(row if self.base is None else (self.base, row))

    def load(self, f, j, i, off=0):
        return self.ref[f, j, self.at(i, off), :]

    def store(self, f, j, i, x):
        self.ref[f, j, self.at(i), :] = x


class Sweep:
    def __init__(self, tiles, turned):
        self.n, self.turned = tiles, turned
        self.first, self.last = iota(1) == 0, iota(1) == LANE - 1

    def spread(self, ve, vx, i):
        for f in (Q, R):
            xs = shift([ve.load(f, j, i) for j in range(self.n)], 1, self.first, self.last)
            for j, x in enumerate(xs):
                vx.store(f, j, i, x)

    def stress(self, ve, vx, old, new, par, i):
        keep = 1.0 / (1.0 + relax_rate)
        for j in range(self.n):
            q, r, qx, rx = (v.load(f, j, i) for v in (ve, vx) for f in (Q, R))
            qa, ra, qxa, rxa = (v.load(f, j, i, -1) for v in (ve, vx) for f in (Q, R))
            a, b = q - qxa, rx - ra
            if self.turned:
                d, s = a - b, a + b
                t = (r - rxa) - (qx - qa)
            else:
                d, s = a + b, a - b
                t = (r - rxa) + (qx - qa)
            e = (d * d + 4.0 * delta_floor * delta_floor) + 0.25 * (t * t + s * s)
            pr = par.load(PR, j, i)
            g = pr * lax.rsqrt(e)
            h = 0.25 * g
            push, side = g * d - pr, h * s
            new.store(AL, j, i, old.load(AL, j, i) * keep + (push + side))
            new.store(BE, j, i, old.load(BE, j, i) * keep + (push - side))
            new.store(S2, j, i, old.load(S2, j, i) * keep + h * t)

    def force(self, ss, frc, i):
        a, c = [], []
        for j in range(self.n):
            ad, s, sd, b = ss.load(AL, j, i, 1), ss.load(S2, j, i), ss.load(S2, j, i, 1), ss.load(BE, j, i)
            if self.turned:
                a.append(ad + s)
                c.append(sd + b)
            else:
                a.append(ad - s)
                c.append(sd - b)
        for f, xs in ((0, a), (1, c)):
            for j, x in enumerate(shift(xs, -1, self.first, self.last)):
                frc.store(f, j, i, x)

    def velocity(self, old, new, ss, frc, par, i):
        for j in range(self.n):
            al, s, sd, bd = ss.load(AL, j, i), ss.load(S2, j, i), ss.load(S2, j, i, 1), ss.load(BE, j, i, 1)
            fa, fc = frc.load(0, j, i), frc.load(1, j, i)
            if self.turned:
                fq, fr = fa - (sd + al), fc - (bd + s)
            else:
                fq, fr = fa + (sd - al), fc + (bd - s)
            q, r, m = old.load(Q, j, i), old.load(R, j, i), par.load(M, j, i)
            x = m * q + (fq + par.load(TQ, j, i))
            y = m * r + (fr + par.load(TR, j, i))
            ca, cb = par.load(CA, j, i), par.load(CB, j, i)
            new.store(Q, j, i, ca * x - cb * y)
            new.store(R, j, i, ca * y + cb * x)

    def reduce(self, old, new, par, i, add):
        for j in range(self.n):
            nq, nr = new.load(Q, j, i), new.load(R, j, i)
            dq, dr = nq - old.load(Q, j, i), nr - old.load(R, j, i)
            add(j, dq * dq + dr * dr, par.load(M, j, i) * (nq * nq + nr * nr))


class Stream:
    def __init__(self, sw, ve, vx, ss, frc, par, rows):
        self.sw, self.ve, self.vx, self.ss, self.frc, self.par, self.rows = sw, ve, vx, ss, frc, par, rows

    def step(self, p, stages):
        sw, rows, unit = self.sw, self.rows, 8 * UN
        row = pl.multiple_of(p * unit, unit)
        turn = pl.multiple_of(lax.rem(row, rows), unit)
        late = pl.multiple_of(lax.rem(row + rows - 4 * unit, rows), unit)
        slots = [View(self.frc, PAD, pl.multiple_of(lax.rem(p + k, 2) * unit, unit)) for k in (0, 1)]
        was = lambda ref, lag: View(ref, FRONT - lag * unit, row)
        now = lambda ref, lag: View(ref, FRONT + rows - lag * unit, row)
        par = lambda lag: View(self.par, FRONT - lag * unit, turn)
        ve, ss = self.ve, self.ss
        todo = {
            "velocity": (was(ve, 3), now(ve, 3), now(ss, 3), slots[1], par(3)),
            "force": (now(ss, 2), slots[0]),
            "stress": (was(ve, 0), View(self.vx, PAD, turn), was(ss, 0), now(ss, 0), par(0)),
            "spread": (now(ve, 4), View(self.vx, PAD, late)),
        }
        for name in stages:
            for i in range(UN):
                getattr(sw, name)(*todo[name], i)

    def run(self, lo, hi):
        every = ("velocity", "force", "stress", "spread")
        steps = ITERS * self.rows // (8 * UN)
        for a, b, stages in (
            (0, 2, every[2:3]), (2, 3, every[1:3]), (3, 4, every[:3]),
            (4, steps, every), (steps, steps + 2, every[:2]), (steps + 2, steps + 3, every[:1]),
        ):
            if isinstance(lo, int):
                a, b = max(a, lo), min(b, hi)
                if a >= b:
                    continue
            elif a != 4:
                continue
            else:
                a, b = lo, hi

            def body(p, carry):
                self.step(p, stages)
                return carry

            lax.fori_loop(a, b, body, 0)


def core_kernel(
    nx, ny, rows, cols,
    vel, stress, strength, mass, wind, current, mask, water,
    vel_out, stress_out, total_out,
    strength_v, mass_v, mask_v, water_v, wind_v, current_v,
    ve, vx, ss, frc, par, acc,
    pack_u, pack_d, recv_u, recv_d, own_l, own_r, recv_l, recv_r,
    corner_u, corner_d, corner_in,
    row_va, row_vb, row_sa, row_sb, row_x, row_f, row_p, col_va, col_vb, col_sa, col_sb, col_x, col_f, col_p,
    packed, edge_t, edge, mine, slots,
    load_sem, send_sem, recv_sem, sum_sem,
):
    ix = lax.axis_index("gx")
    iy = lax.axis_index("gy")
    n, tall, blocks = cols // LANE, rows // LANE, rows // 8
    chunks = 8
    per = rows // chunks
    lane, sub = iota(1), iota(0)
    zero = jnp.zeros((8, LANE), f32)

    def loads(c):
        part = pl.ds(pl.multiple_of(c * per, 8), per)
        later = pl.ds(pl.multiple_of(c * per + FRONT, 8), per)
        both = slice(None)
        pairs = [
            (strength.at[part], strength_v.at[part]),
            (mass.at[part], mass_v.at[part]),
            (mask.at[part], mask_v.at[part]),
            (water.at[part], water_v.at[part]),
            (wind.at[both, part], wind_v.at[both, part]),
            (current.at[both, part], current_v.at[both, part]),
        ]
        for j in range(n):
            tile = pl.ds(j * LANE, LANE)
            pairs.append((vel.at[both, part, tile], ve.at[both, j, later]))
            pairs.append((stress.at[both, part, tile], ss.at[both, j, later]))
        return [pltpu.make_async_copy(a, b, load_sem.at[c, k]) for k, (a, b) in enumerate(pairs)]

    for c in [0, chunks - 1] + list(range(1, chunks - 1)):
        for cp in loads(c):
            cp.start()

    count = nx * ny
    me = ix * ny + iy

    def others(act):
        def line(k, carry):
            x = lax.rem(ix + nx // 2 + k, nx)
            for m in range(ny):
                y = lax.rem(iy + ny // 2 + m, ny)

                @pl.when((x != ix) | (y != iy))
                def _():
                    act(x, y)
            return carry

        lax.fori_loop(0, nx, line, 0)

    barrier = pltpu.get_barrier_semaphore()
    others(lambda x, y: pl.semaphore_signal(barrier, inc=1, device_id=(x, y), device_id_type=MESH))

    for j in range(n):
        for f in range(2):
            ve[f, j, FRONT - 8 : FRONT, :] = zero
            vx[f, j, 0:8, :] = zero
        for f in range(3):
            ss[f, j, FRONT + (ITERS + 1) * rows : FRONT + (ITERS + 1) * rows + 8, :] = zero
    for st in (row_va, row_vb, row_sa, row_sb, row_x, col_va, col_vb, col_sa, col_sb, col_x):
        for side in range(2):
            for f in range(st.shape[1]):
                for j in range(st.shape[2]):
                    st[side, f, j, 0:8, :] = zero
                    st[side, f, j, 24:32, :] = zero

    sw = Sweep(n, False)

    def prepare(base, i):
        rowsl, at = rows8((base, 8 * i)), rows8((base, 8 * i + FRONT))
        ends = []
        for j in range(n):
            src = (rowsl, slice(j * LANE, (j + 1) * LANE))
            w = mask_v[src].astype(f32) * (1.0 - water_v[src].astype(f32))
            m = mass_v[src]
            inertia = m * (1.0 / time_step)
            diagonal = inertia + drag_coef
            turning = m * coriolis
            scale = (0.5 * w) / (diagonal * diagonal + turning * turning)
            tx = wind_v[(0,) + src] + drag_coef * current_v[(0,) + src]
            ty = wind_v[(1,) + src] + drag_coef * current_v[(1,) + src]
            u, v = ve[0, j, at, :], ve[1, j, at, :]
            s1, s2, s12 = (ss[f, j, at, :] for f in range(3))
            t = s12 + s12
            q, r = u + v, u - v
            moving = {Q: q, R: r}
            state = {AL: s1 + t, BE: s1 - t, S2: s2}
            fixed = {
                PR: strength_v[src] * w * (relax_rate / (1.0 + relax_rate)),
                M: inertia * 2.0,
                TQ: (tx + ty) * 2.0,
                TR: (tx - ty) * 2.0,
                CA: diagonal * scale,
                CB: turning * scale,
            }
            for f, x in moving.items():
                ve[f, j, at, :] = x
            for f, x in ((AL, state[AL]), (BE, state[BE])):
                ss[f, j, at, :] = x
            for f, x in fixed.items():
                par[f, j, at, :] = x
            if j in (0, n - 1):
                ends.append([(moving, state, fixed)[a][f] for a, f in SENT])
        low, high = ends[0], ends[-1]
        packs = [zero, zero]
        for i in range(NF):
            x = roll(select(lane < LANE // 2, low[i], high[i]), 16 * (i % 8) + 8, 1)
            g = (lane >= 16 * (i % 8)) & (lane < 16 * (i % 8) + 16)
            packs[i // 8] = select(g, x, packs[i // 8])
        for i in range(2):
            packed[i, rowsl, :] = packs[i]

    group = min(8, per // 8)

    def prepare_chunk(c):
        for cp in loads(c):
            cp.wait()

        def body(p, carry):
            base = pl.multiple_of(c * per + p * (8 * group), 8 * group)
            for i in range(group):
                prepare(base, i)
            for i in range(group):
                sw.spread(View(ve, FRONT, base), View(vx, PAD, base), i)
            return carry

        lax.fori_loop(0, per // 8 // group, body, 0)

    def exists(d):
        return (ix + d[0] >= 0) & (ix + d[0] < nx) & (iy + d[1] >= 0) & (iy + d[1] < ny)

    def message(d, which):
        k = DIRS.index(d)
        dx, dy = d
        out = []
        if which == 1:
            pass
        elif dy == 0:
            out.append((pack_u, recv_d, k) if dx < 0 else (pack_d, recv_u, k))
        elif dx == 0:
            out.append((own_l, recv_r, k) if dy < 0 else (own_r, recv_l, k))
        if dx and which != 0:
            c = CORNERS.index(d)
            back = CORNERS.index((-dx, -dy))
            out.append((corner_u if dx < 0 else corner_d, corner_in.at[back], 4 + c))
        return [
            pltpu.make_async_remote_copy(
                src_ref=a, dst_ref=b, send_sem=send_sem.at[s], recv_sem=recv_sem.at[s],
                device_id=(ix + dx, iy + dy), device_id_type=MESH,
            )
            for a, b, s in out
        ]

    def plane(i, j, block):
        a, f = SENT[i]
        row = block * 8 + FRONT
        return (ve, ss, par)[a][f, j, row : row + 8, :]

    prepare_chunk(0)
    prepare_chunk(chunks - 1)
    for g in range(PAIRS):
        i0, i1 = 2 * g, min(2 * g + 1, NF - 1)
        for j in range(n):
            pack_u[g, j] = select(sub < 4, plane(i0, j, 0), roll(plane(i1, j, 0), 4, 0))
            pack_d[g, j] = select(sub < 4, roll(plane(i0, j, blocks - 1), 4, 0), plane(i1, j, blocks - 1))
    pl.semaphore_wait(barrier, count - 1)
    for d in DIRS[:2]:
        @pl.when(exists(d))
        def _():
            message(d, 0)[0].start()

    for i in range(NF):
        a, f = SENT[i]
        dst = (row_va, row_sa, row_p)[a]
        for j in range(n):
            x, y = (roll(plane(i, j, b), 4, 0) for b in (0, 1))
            dst[0, f, j, 8:16, :] = x
            dst[0, f, j, 16:24, :] = select(sub < 4, x, y)
            x, y = (roll(plane(i, j, b), 4, 0) for b in (blocks - 2, blocks - 1))
            dst[1, f, j, 8:16, :] = select(sub < 4, x, y)
            dst[1, f, j, 16:24, :] = y

    stream = Stream(sw, ve, vx, ss, frc, par, rows)
    pace = per // (8 * UN)
    begin = 1
    if pace:
        stream.run(0, pace)
        while begin < chunks - 1 and begin * pace < 4:
            prepare_chunk(begin)
            stream.run(begin * pace, (begin + 1) * pace)
            begin += 1

    def advance(c, carry):
        prepare_chunk(c)
        if pace:
            stream.run(c * pace, (c + 1) * pace)
        return carry

    lax.fori_loop(begin, chunks - 1, advance, 0)

    def wrap(i, carry):
        for f in range(6):
            for j in range(n):
                par[f, j, rows8((8 * i, FRONT - 24 * UN)), :] = par[f, j, rows8((8 * i, FRONT + rows - 24 * UN)), :]
        return carry

    lax.fori_loop(0, 3 * UN, wrap, 0)

    for i in range(2):
        for t in range(tall):
            x = packed[i, t * LANE : (t + 1) * LANE, :].T
            for f in range(8 * i, min(8 * i + 8, NF)):
                o = 16 * (f - 8 * i)
                own_r[f, t] = x[o : o + 8]
                own_l[f, t] = x[o + 8 : o + 16]
                a, g = SENT[f]
                dst = (col_va, col_sa, col_p)[a]
                dst[0, g, t, 16:24, :] = x[o + 8 : o + 16]
                dst[1, g, t, 8:16, :] = x[o : o + 8]
    up, down = zero, zero
    for i in range(2 * NF):
        src = own_l if i < NF else own_r
        g = (lane >= 4 * i) & (lane < 4 * i + 4)
        up = select(g, roll(src[i % NF, 0], 4 * i, 1), up)
        down = select(g, roll(src[i % NF, tall - 1], 4 * i + 4, 1), down)
    corner_u[...] = up
    corner_d[...] = down
    for d in DIRS[2:4]:
        @pl.when(exists(d))
        def _():
            message(d, 0)[0].start()
    for d in CORNERS:
        @pl.when(exists(d))
        def _():
            message(d, 1)[0].start()

    stream.run((chunks - 1) * pace, ITERS * blocks // UN + 3)

    def clear(ref, lead):
        for i in lead:
            ref[i] = jnp.zeros(ref.shape[1:], f32)

    for d, buf in (((-1, 0), recv_u), ((1, 0), recv_d), ((0, -1), recv_l), ((0, 1), recv_r)):
        @pl.when(~exists(d))
        def _():
            clear(buf, range(buf.shape[0]))

    for c, d in enumerate(CORNERS):
        @pl.when(~exists(d))
        def _():
            corner_in[c] = zero

    for d in DIRS:
        @pl.when(exists(d))
        def _():
            for cp in message((-d[0], -d[1]), 2):
                cp.wait_recv()
            for cp in message(d, 2):
                cp.wait_send()

    for i in range(NF):
        a, f = SENT[i]
        dst = (row_va, row_sa, row_p)[a]
        g, odd = divmod(i, 2)
        for j in range(n):
            x, y = recv_u[g, j], recv_d[g, j]
            x = roll(x, 4, 0) if odd else x
            y = y if odd else roll(y, 4, 0)
            dst[0, f, j, 8:16, :] = select(sub < 4, x, dst[0, f, j, 8:16, :])
            dst[1, f, j, 16:24, :] = select(sub < 4, dst[1, f, j, 16:24, :], y)
        dst = (col_va, col_sa, col_p)[a]
        for t in range(tall):
            dst[0, f, t, 8:16, :] = recv_l[i, t]
            dst[1, f, t, 16:24, :] = recv_r[i, t]

        def corner(u, d, at):
            x = roll(corner_in[CORNERS.index(u)], LANE - 4 - 4 * at, 1)
            y = roll(corner_in[CORNERS.index(d)], -4 * at, 1)
            return select(lane < 4, y, select(lane >= LANE - 4, x, zero))

        dst[0, f, tall, 8:16, :] = corner((-1, -1), (1, -1), NF + i)
        dst[0, f, tall, 16:24, :] = corner((-1, 0), (1, 0), i)
        dst[1, f, tall, 8:16, :] = corner((-1, 0), (1, 0), NF + i)
        dst[1, f, tall, 16:24, :] = corner((-1, 1), (1, 1), i)

    strips = []
    for s, va, vb, sa, sb, x, fr, p in (
        (sw, row_va, row_vb, row_sa, row_sb, row_x, row_f, row_p),
        (Sweep(tall + 1, True), col_va, col_vb, col_sa, col_sb, col_x, col_f, col_p),
    ):
        for i in range(2):
            strips.append((s, i, *(View(y.at[i]) for y in (va, vb, sa, sb, x, fr, p))))

    def strip_cycles(t, carry):
        for flip in (False, True):
            for s, i, va, vb, sa, sb, x, fr, p in strips:
                for k in range(2):
                    s.spread(vb if flip else va, x, k)
            for s, i, va, vb, sa, sb, x, fr, p in strips:
                for k in range(2):
                    s.stress(vb if flip else va, x, *((sb, sa) if flip else (sa, sb)), p, k)
            for s, i, va, vb, sa, sb, x, fr, p in strips:
                for k in range(2):
                    s.force(sa if flip else sb, fr, k)
            for s, i, va, vb, sa, sb, x, fr, p in strips:
                for k in range(2):
                    s.velocity(*((vb, va, sa) if flip else (va, vb, sb)), fr, p, k)
        return carry

    lax.fori_loop(0, ITERS // 2, strip_cycles, 0)
    row_e, col_e = (row_va, row_sa), (col_va, col_sa)
    sums = [[zero, zero] for _ in range(n)]
    more = [zero, zero]
    for s, i, va, vb, sa, sb, x, fr, p in strips:
        for k in range(2):
            def add(j, x, y):
                if s.turned and (j == tall or k == i):
                    return
                good = sub >= 4 if k == 0 else sub < 4
                box = more if s.turned else sums[j]
                box[0] += select(good, x, zero)
                box[1] += select(good, y, zero)

            s.reduce(vb, va, p, k, add)

    last = FRONT + ITERS * rows
    acc[...] = jnp.zeros_like(acc)

    def reduce_rows(p, group, lead):
        part = {}

        def add(j, x, y):
            for i, z in ((2 * j, x), (2 * j + 1, y)):
                part[i] = part[i] + z if i in part else z

        base = pl.multiple_of(p * (8 * group), 8 * group)
        for i in range(group):
            sw.reduce(View(ve, last - rows + lead, base), View(ve, last + lead, base), View(par, FRONT + lead, base), i, add)
        for i, z in part.items():
            acc[i] += z

    lax.fori_loop(0, (blocks - 2) // 2, lambda p, c: (reduce_rows(p, 2, 8), c)[1], 0)

    for j in range(n):
        good = lane >= 4 if j == 0 else lane < LANE - 4 if j == n - 1 else None
        if n == 1:
            good = (lane >= 4) & (lane < LANE - 4)
        for i in range(2):
            x = acc[2 * j + i] + sums[j][i]
            more[i] += x if good is None else jnp.where(good, x, 0.0)
    x, y = (jnp.sum(m, axis=0, keepdims=True) for m in more)
    x, y = x + roll(x, LANE // 2, 1), y + roll(y, LANE // 2, 1)
    half = lax.broadcasted_iota(jnp.int32, (1, LANE), 1) < LANE // 2
    part = jnp.where(half, x, y)
    mine[...] = part

    def sum_copy(x, y):
        return pltpu.make_async_remote_copy(
            src_ref=mine, dst_ref=slots.at[me], send_sem=sum_sem.at[0], recv_sem=sum_sem.at[1],
            device_id=(x, y), device_id_type=MESH,
        )

    others(lambda x, y: sum_copy(x, y).start())
    slots[pl.ds(me, 1)] = part[None]

    for t in range(tall):
        for o, (a, f) in enumerate(SENT[:5]):
            x = select(sub < 4, col_e[a][0, f, t, 16:24, :], col_e[a][1, f, t, 8:16, :])
            edge_t[t, o * 8 : o * 8 + 8, :] = roll(x, 4, 0)
    for t in range(tall):
        edge[t * LANE : (t + 1) * LANE, :] = edge_t[t].T

    def emit(rowsl, src):
        ev = edge[rowsl, :]
        es = [roll(ev, LANE - 4 - 8 * o, 1) for o in range(5)]
        for j in range(n):
            vals = [src[a][0][f, j, src[a][1], :] for a, f in SENT[:5]]
            if j == 0:
                vals = [select(lane < 4, e, x) for e, x in zip(es, vals)]
            if j == n - 1:
                vals = [select(lane >= LANE - 4, e, x) for e, x in zip(es, vals)]
            q, r, al, be, s2 = vals
            c = slice(j * LANE, (j + 1) * LANE)
            vel_out[0, rowsl, c] = 0.5 * (q + r)
            vel_out[1, rowsl, c] = 0.5 * (q - r)
            stress_out[0, rowsl, c] = 0.5 * (al + be)
            stress_out[1, rowsl, c] = s2
            stress_out[2, rowsl, c] = 0.25 * (al - be)

    def row_strip(i):
        return [(x.at[i], slice(12, 20)) for x in row_e]

    emit(slice(0, 8), row_strip(0))
    emit(slice(rows - 8, rows), row_strip(1))

    def emit_rows(base, count):
        for i in range(1, count + 1):
            at = rows8((base, 8 * i + last))
            emit(rows8((base, 8 * i)), [(ve, at), (ss, at)])

    batch = min(10, blocks - 2)

    def body(p, c):
        emit_rows(pl.multiple_of(p * (8 * batch), 8), batch)
        return c

    lax.fori_loop(0, (blocks - 2) // batch, body, 0)
    emit_rows((blocks - 2) // batch * batch * 8, (blocks - 2) % batch)

    for i in range(2):
        most = slots.at[pl.ds(0, count - 1)]
        pltpu.make_async_copy(most, most, sum_sem.at[i]).wait()
    total = [slots[i] for i in range(count)]
    while len(total) > 1:
        total = [a + b for a, b in zip(total[::2], total[1::2])] + total[len(total) // 2 * 2 :]
    total = total[0]
    scale = 1.0 / (rows * nx * cols * ny)
    x = jnp.sum(jnp.where(half, total, 0.0), axis=1, keepdims=True) * (0.5 * scale)
    y = jnp.sum(jnp.where(half, 0.0, total), axis=1, keepdims=True) * (0.0625 * scale)
    total_out[...] = jnp.where(half, x, y)


def write_kernel(vel, stress, total, new_vel, new_stress, residual, kinetic, res, kin, sem, few):
    copies = [
        pltpu.make_async_copy(a.at[f, part], b.at[f, part], sem.at[k, f, h])
        for k, (a, b) in enumerate(((vel, new_vel), (stress, new_stress)))
        for f in range(a.shape[0])
        for h, part in enumerate((pl.ds(0, a.shape[1] // 2), pl.ds(a.shape[1] // 2, a.shape[1] // 2)))
    ]
    for c in copies:
        c.start()
    x = total[...]
    res[0, 0] = x[0, 0]
    kin[0, 0] = x[0, LANE - 1]
    for i, (a, b) in enumerate(((res, residual), (kin, kinetic))):
        copies.append(pltpu.make_async_copy(a, b, few.at[i]))
        copies[-1].start()
    for c in copies:
        c.wait()


def per_device(nx, ny, velocity, stress, strength, ice_mass, wind, current, ice_mask, open_water):
    _, rows, cols = velocity.shape
    n, tall, strip = cols // LANE, rows // LANE, rows + 2 * PAD
    i32 = jnp.int32
    vmem = pl.BlockSpec(memory_space=pltpu.VMEM)
    hbm = pl.BlockSpec(memory_space=pl.ANY)
    dma = pltpu.SemaphoreType.DMA
    V = pltpu.VMEM
    count = nx * ny
    new_vel, new_stress, total = pl.pallas_call(
        functools.partial(core_kernel, nx, ny, rows, cols),
        out_shape=(V((2, rows, cols), f32), V((3, rows, cols), f32), V((1, LANE), f32)),
        in_specs=[pl.BlockSpec(memory_space=pltpu.HBM)] * 8,
        out_specs=(vmem, vmem, vmem),
        scratch_shapes=[
            V((rows, cols), f32), V((rows, cols), f32), V((rows, cols), i32), V((rows, cols), i32),
            V((2, rows, cols), f32), V((2, rows, cols), f32),
            V((2, n, FRONT + (ITERS + 1) * rows + 8, LANE), f32), V((2, n, rows + PAD, LANE), f32),
            V((3, n, FRONT + (ITERS + 1) * rows + 8, LANE), f32), V((2, n, 2 * 8 * UN + PAD, LANE), f32),
            V((6, n, FRONT + rows + 8, LANE), f32), V((2 * n, 8, LANE), f32),
            V((PAIRS, n, 8, LANE), f32), V((PAIRS, n, 8, LANE), f32),
            V((PAIRS, n, 8, LANE), f32), V((PAIRS, n, 8, LANE), f32),
            V((NF, tall, 8, LANE), f32), V((NF, tall, 8, LANE), f32),
            V((NF, tall, 8, LANE), f32), V((NF, tall, 8, LANE), f32),
            V((8, LANE), f32), V((8, LANE), f32), V((6, 8, LANE), f32),
            V((2, 2, n, 32, LANE), f32), V((2, 2, n, 32, LANE), f32),
            V((2, 3, n, 32, LANE), f32), V((2, 3, n, 32, LANE), f32), V((2, 2, n, 32, LANE), f32),
            V((2, 2, n, 32, LANE), f32), V((2, 6, n, 32, LANE), f32),
            V((2, 2, tall + 1, 32, LANE), f32), V((2, 2, tall + 1, 32, LANE), f32),
            V((2, 3, tall + 1, 32, LANE), f32), V((2, 3, tall + 1, 32, LANE), f32), V((2, 2, tall + 1, 32, LANE), f32),
            V((2, 2, tall + 1, 32, LANE), f32), V((2, 6, tall + 1, 32, LANE), f32),
            V((2, rows, LANE), f32), V((tall, LANE, LANE), f32), V((rows, LANE), f32),
            V((1, LANE), f32), V((count, 1, LANE), f32),
            dma((8, 6 + 2 * n)), dma((10,)), dma((10,)), dma((2,)),
        ],
        compiler_params=pltpu.CompilerParams(
            collective_id=0, has_side_effects=True, vmem_limit_bytes=57 << 20
        ),
        name="core",
    )(
        *[
            pltpu.with_memory_space_constraint(x, pltpu.HBM)
            for x in (velocity, stress, strength, ice_mass, wind, current, ice_mask, open_water)
        ]
    )
    new_vel, new_stress, residual, kinetic = pl.pallas_call(
        write_kernel,
        out_shape=(
            jax.ShapeDtypeStruct(velocity.shape, f32),
            jax.ShapeDtypeStruct(stress.shape, f32),
            jax.ShapeDtypeStruct((1, 1), f32),
            jax.ShapeDtypeStruct((1, 1), f32),
        ),
        in_specs=[vmem, vmem, vmem],
        out_specs=(hbm,) * 4,
        scratch_shapes=[pltpu.SMEM((1, 1), f32), pltpu.SMEM((1, 1), f32), dma((2, 3, 2)), dma((2,))],
        compiler_params=pltpu.CompilerParams(vmem_limit_bytes=1 << 20),
        name="write",
    )(new_vel, new_stress, total)
    return new_vel, new_stress, residual.reshape(()), kinetic.reshape(())


def solution(mesh):
    two, three = P("gx", "gy"), P(None, "gx", "gy")
    return jax.shard_map(
        functools.partial(per_device, mesh.shape["gx"], mesh.shape["gy"]),
        mesh=mesh,
        in_specs=(three, three, two, two, three, three, two, two),
        out_specs=(three, three, P(), P()),
        check_vma=False,
    )
```

```python
import functools

import jax
import jax.numpy as jnp
from jax import lax
from jax.experimental import pallas as pl
from jax.experimental.pallas import tpu as pltpu
from jax.sharding import PartitionSpec as P

ITERS = 4
relax_rate = 0.8
time_step = 0.5
drag_coef = 1.0
coriolis = 0.3
delta_floor = 0.05
MESH = pl.DeviceIdType.MESH

Q, R = range(2)
AL, S2, BE = range(3)
PR, M, TQ, TR, CA, CB = range(6)
SENT = ((0, Q), (0, R), (1, AL), (1, BE), (1, S2)) + tuple((2, f) for f in range(6))
NF = len(SENT)
PAIRS = (NF + 1) // 2
LANE = 128
PAD = 8
FRONT = 128
UN = 4
DIRS = ((-1, 0), (1, 0), (0, -1), (0, 1), (-1, -1), (-1, 1), (1, -1), (1, 1))
CORNERS = ((-1, 0), (1, 0)) + DIRS[4:]
f32 = jnp.float32


def iota(axis):
    return lax.broadcasted_iota(jnp.int32, (8, LANE), axis)


def roll(x, by, axis):
    by %= x.shape[axis]
    return pltpu.roll(x, by, axis=axis) if by else x


def rows8(row):
    if isinstance(row, int):
        return slice(row, row + 8)
    base, off = row
    return pl.ds(base + off if off % 8 else pl.multiple_of(base + off, 8), 8)


def select(mask, x, y):
    return lax.select(mask, x, y)


def shift(xs, by, first, last):
    n = len(xs)
    turned = [roll(x, by, 1) for x in xs]
    if by > 0:
        return [select(first, turned[(j - 1) % n], turned[j]) for j in range(n)]
    return [select(last, turned[(j + 1) % n], turned[j]) for j in range(n)]


class View:
    def __init__(self, ref, pad=PAD, base=None):
        self.ref, self.pad, self.base = ref, pad, base

    def at(self, i, off=0):
        row = self.pad + 8 * i + off
        return rows8(row if self.base is None else (self.base, row))

    def load(self, f, j, i, off=0):
        return self.ref[f, j, self.at(i, off), :]

    def store(self, f, j, i, x):
        self.ref[f, j, self.at(i), :] = x


class Sweep:
    def __init__(self, tiles, turned):
        self.n, self.turned = tiles, turned
        self.first, self.last = iota(1) == 0, iota(1) == LANE - 1

    def spread(self, ve, vx, i):
        for f in (Q, R):
            xs = shift([ve.load(f, j, i) for j in range(self.n)], 1, self.first, self.last)
            for j, x in enumerate(xs):
                vx.store(f, j, i, x)

    def stress(self, ve, vx, old, new, par, i):
        keep = 1.0 / (1.0 + relax_rate)
        for j in range(self.n):
            q, r, qx, rx = (v.load(f, j, i) for v in (ve, vx) for f in (Q, R))
            qa, ra, qxa, rxa = (v.load(f, j, i, -1) for v in (ve, vx) for f in (Q, R))
            a, b = q - qxa, rx - ra
            if self.turned:
                d, s = a - b, a + b
                t = (r - rxa) - (qx - qa)
            else:
                d, s = a + b, a - b
                t = (r - rxa) + (qx - qa)
            e = (d * d + 4.0 * delta_floor * delta_floor) + 0.25 * (t * t + s * s)
            pr = par.load(PR, j, i)
            g = pr * lax.rsqrt(e)
            h = 0.25 * g
            push, side = g * d - pr, h * s
            new.store(AL, j, i, old.load(AL, j, i) * keep + (push + side))
            new.store(BE, j, i, old.load(BE, j, i) * keep + (push - side))
            new.store(S2, j, i, old.load(S2, j, i) * keep + h * t)

    def force(self, ss, frc, i):
        a, c = [], []
        for j in range(self.n):
            ad, s, sd, b = ss.load(AL, j, i, 1), ss.load(S2, j, i), ss.load(S2, j, i, 1), ss.load(BE, j, i)
            if self.turned:
                a.append(ad + s)
                c.append(sd + b)
            else:
                a.append(ad - s)
                c.append(sd - b)
        for f, xs in ((0, a), (1, c)):
            for j, x in enumerate(shift(xs, -1, self.first, self.last)):
                frc.store(f, j, i, x)

    def velocity(self, old, new, ss, frc, par, i):
        for j in range(self.n):
            al, s, sd, bd = ss.load(AL, j, i), ss.load(S2, j, i), ss.load(S2, j, i, 1), ss.load(BE, j, i, 1)
            fa, fc = frc.load(0, j, i), frc.load(1, j, i)
            if self.turned:
                fq, fr = fa - (sd + al), fc - (bd + s)
            else:
                fq, fr = fa + (sd - al), fc + (bd - s)
            q, r, m = old.load(Q, j, i), old.load(R, j, i), par.load(M, j, i)
            x = m * q + (fq + par.load(TQ, j, i))
            y = m * r + (fr + par.load(TR, j, i))
            ca, cb = par.load(CA, j, i), par.load(CB, j, i)
            new.store(Q, j, i, ca * x - cb * y)
            new.store(R, j, i, ca * y + cb * x)

    def reduce(self, old, new, par, i, add):
        for j in range(self.n):
            nq, nr = new.load(Q, j, i), new.load(R, j, i)
            dq, dr = nq - old.load(Q, j, i), nr - old.load(R, j, i)
            add(j, dq * dq + dr * dr, par.load(M, j, i) * (nq * nq + nr * nr))


class Stream:
    def __init__(self, sw, ve, vx, ss, frc, par, rows):
        self.sw, self.ve, self.vx, self.ss, self.frc, self.par, self.rows = sw, ve, vx, ss, frc, par, rows

    def step(self, p, stages):
        sw, rows, unit = self.sw, self.rows, 8 * UN
        row = pl.multiple_of(p * unit, unit)
        turn = pl.multiple_of(lax.rem(row, rows), unit)
        late = pl.multiple_of(lax.rem(row + rows - 4 * unit, rows), unit)
        slots = [View(self.frc, PAD, pl.multiple_of(lax.rem(p + k, 2) * unit, unit)) for k in (0, 1)]
        was = lambda ref, lag: View(ref, FRONT - lag * unit, row)
        now = lambda ref, lag: View(ref, FRONT + rows - lag * unit, row)
        par = lambda lag: View(self.par, FRONT - lag * unit, turn)
        ve, ss = self.ve, self.ss
        todo = {
            "velocity": (was(ve, 3), now(ve, 3), now(ss, 3), slots[1], par(3)),
            "force": (now(ss, 2), slots[0]),
            "stress": (was(ve, 0), View(self.vx, PAD, turn), was(ss, 0), now(ss, 0), par(0)),
            "spread": (now(ve, 4), View(self.vx, PAD, late)),
        }
        for name in stages:
            for i in range(UN):
                getattr(sw, name)(*todo[name], i)

    def run(self, lo, hi):
        every = ("velocity", "force", "stress", "spread")
        steps = ITERS * self.rows // (8 * UN)
        for a, b, stages in (
            (0, 2, every[2:3]), (2, 3, every[1:3]), (3, 4, every[:3]),
            (4, steps, every), (steps, steps + 2, every[:2]), (steps + 2, steps + 3, every[:1]),
        ):
            if isinstance(lo, int):
                a, b = max(a, lo), min(b, hi)
                if a >= b:
                    continue
            elif a != 4:
                continue
            else:
                a, b = lo, hi

            def body(p, carry):
                self.step(p, stages)
                return carry

            lax.fori_loop(a, b, body, 0)


def core_kernel(
    nx, ny, rows, cols,
    vel, stress, strength, mass, wind, current, mask, water,
    vel_out, stress_out, total_out,
    strength_v, mass_v, mask_v, water_v, wind_v, current_v,
    ve, vx, ss, frc, par, acc,
    pack_u, pack_d, recv_u, recv_d, own_l, own_r, recv_l, recv_r,
    corner_u, corner_d, corner_in,
    row_va, row_vb, row_sa, row_sb, row_x, row_f, row_p, col_va, col_vb, col_sa, col_sb, col_x, col_f, col_p,
    packed, edge_t, edge, mine, slots,
    load_sem, send_sem, recv_sem, sum_sem,
):
    ix = lax.axis_index("gx")
    iy = lax.axis_index("gy")
    n, tall, blocks = cols // LANE, rows // LANE, rows // 8
    chunks = 8
    per = rows // chunks
    lane, sub = iota(1), iota(0)
    zero = jnp.zeros((8, LANE), f32)

    def loads(c):
        part = pl.ds(pl.multiple_of(c * per, 8), per)
        later = pl.ds(pl.multiple_of(c * per + FRONT, 8), per)
        both = slice(None)
        pairs = [
            (strength.at[part], strength_v.at[part]),
            (mass.at[part], mass_v.at[part]),
            (mask.at[part], mask_v.at[part]),
            (water.at[part], water_v.at[part]),
            (wind.at[both, part], wind_v.at[both, part]),
            (current.at[both, part], current_v.at[both, part]),
        ]
        for j in range(n):
            tile = pl.ds(j * LANE, LANE)
            pairs.append((vel.at[both, part, tile], ve.at[both, j, later]))
            pairs.append((stress.at[both, part, tile], ss.at[both, j, later]))
        return [pltpu.make_async_copy(a, b, load_sem.at[c]) for a, b in pairs]

    for c in [0, chunks - 1] + list(range(1, chunks - 1)):
        for cp in loads(c):
            cp.start()

    count = nx * ny
    me = ix * ny + iy

    def others(act):
        def line(k, carry):
            x = lax.rem(ix + nx // 2 + k, nx)
            for m in range(ny):
                y = lax.rem(iy + ny // 2 + m, ny)

                @pl.when((x != ix) | (y != iy))
                def _():
                    act(x, y)
            return carry

        lax.fori_loop(0, nx, line, 0)

    barrier = pltpu.get_barrier_semaphore()
    others(lambda x, y: pl.semaphore_signal(barrier, inc=1, device_id=(x, y), device_id_type=MESH))

    for j in range(n):
        for f in range(2):
            ve[f, j, FRONT - 8 : FRONT, :] = zero
            vx[f, j, 0:8, :] = zero
        for f in range(3):
            ss[f, j, FRONT + (ITERS + 1) * rows : FRONT + (ITERS + 1) * rows + 8, :] = zero
    for st in (row_va, row_vb, row_sa, row_sb, row_x, col_va, col_vb, col_sa, col_sb, col_x):
        for side in range(2):
            for f in range(st.shape[1]):
                for j in range(st.shape[2]):
                    st[side, f, j, 0:8, :] = zero
                    st[side, f, j, 24:32, :] = zero

    sw = Sweep(n, False)

    def prepare(base, i):
        rowsl, at = rows8((base, 8 * i)), rows8((base, 8 * i + FRONT))
        ends = []
        for j in range(n):
            src = (rowsl, slice(j * LANE, (j + 1) * LANE))
            w = mask_v[src].astype(f32) * (1.0 - water_v[src].astype(f32))
            m = mass_v[src]
            inertia = m * (1.0 / time_step)
            diagonal = inertia + drag_coef
            turning = m * coriolis
            scale = (0.5 * w) / (diagonal * diagonal + turning * turning)
            tx = wind_v[(0,) + src] + drag_coef * current_v[(0,) + src]
            ty = wind_v[(1,) + src] + drag_coef * current_v[(1,) + src]
            u, v = ve[0, j, at, :], ve[1, j, at, :]
            s1, s2, s12 = (ss[f, j, at, :] for f in range(3))
            t = s12 + s12
            q, r = u + v, u - v
            moving = {Q: q, R: r}
            state = {AL: s1 + t, BE: s1 - t, S2: s2}
            fixed = {
                PR: strength_v[src] * w * (relax_rate / (1.0 + relax_rate)),
                M: inertia * 2.0,
                TQ: (tx + ty) * 2.0,
                TR: (tx - ty) * 2.0,
                CA: diagonal * scale,
                CB: turning * scale,
            }
            for f, x in moving.items():
                ve[f, j, at, :] = x
            for f, x in ((AL, state[AL]), (BE, state[BE])):
                ss[f, j, at, :] = x
            for f, x in fixed.items():
                par[f, j, at, :] = x
            if j in (0, n - 1):
                ends.append([(moving, state, fixed)[a][f] for a, f in SENT])
        low, high = ends[0], ends[-1]
        packs = [zero, zero]
        for i in range(NF):
            x = roll(select(lane < LANE // 2, low[i], high[i]), 16 * (i % 8) + 8, 1)
            g = (lane >= 16 * (i % 8)) & (lane < 16 * (i % 8) + 16)
            packs[i // 8] = select(g, x, packs[i // 8])
        for i in range(2):
            packed[i, rowsl, :] = packs[i]

    group = min(8, per // 8)

    def prepare_chunk(c):
        size = ve.at[0, :, pl.ds(0, 13 * per)]
        pltpu.make_async_copy(size, size, load_sem.at[c]).wait()

        def body(p, carry):
            base = pl.multiple_of(c * per + p * (8 * group), 8 * group)
            for i in range(group):
                prepare(base, i)
            for i in range(group):
                sw.spread(View(ve, FRONT, base), View(vx, PAD, base), i)
            return carry

        lax.fori_loop(0, per // 8 // group, body, 0)

    def exists(d):
        return (ix + d[0] >= 0) & (ix + d[0] < nx) & (iy + d[1] >= 0) & (iy + d[1] < ny)

    def message(d, which):
        k = DIRS.index(d)
        dx, dy = d
        out = []
        if which == 1:
            pass
        elif dy == 0:
            out.append((pack_u, recv_d, k) if dx < 0 else (pack_d, recv_u, k))
        elif dx == 0:
            out.append((own_l, recv_r, k) if dy < 0 else (own_r, recv_l, k))
        if dx and which != 0:
            c = CORNERS.index(d)
            back = CORNERS.index((-dx, -dy))
            out.append((corner_u if dx < 0 else corner_d, corner_in.at[back], 4 + c))
        return [
            pltpu.make_async_remote_copy(
                src_ref=a, dst_ref=b, send_sem=send_sem.at[s], recv_sem=recv_sem.at[s],
                device_id=(ix + dx, iy + dy), device_id_type=MESH,
            )
            for a, b, s in out
        ]

    def plane(i, j, block):
        a, f = SENT[i]
        row = block * 8 + FRONT
        return (ve, ss, par)[a][f, j, row : row + 8, :]

    prepare_chunk(0)
    prepare_chunk(chunks - 1)
    for g in range(PAIRS):
        i0, i1 = 2 * g, min(2 * g + 1, NF - 1)
        for j in range(n):
            pack_u[g, j] = select(sub < 4, plane(i0, j, 0), roll(plane(i1, j, 0), 4, 0))
            pack_d[g, j] = select(sub < 4, roll(plane(i0, j, blocks - 1), 4, 0), plane(i1, j, blocks - 1))
    pl.semaphore_wait(barrier, count - 1)
    for d in DIRS[:2]:
        @pl.when(exists(d))
        def _():
            message(d, 0)[0].start()

    for i in range(NF):
        a, f = SENT[i]
        dst = (row_va, row_sa, row_p)[a]
        for j in range(n):
            x, y = (roll(plane(i, j, b), 4, 0) for b in (0, 1))
            dst[0, f, j, 8:16, :] = x
            dst[0, f, j, 16:24, :] = select(sub < 4, x, y)
            x, y = (roll(plane(i, j, b), 4, 0) for b in (blocks - 2, blocks - 1))
            dst[1, f, j, 8:16, :] = select(sub < 4, x, y)
            dst[1, f, j, 16:24, :] = y

    stream = Stream(sw, ve, vx, ss, frc, par, rows)
    pace = per // (8 * UN)
    begin = 1
    if pace:
        stream.run(0, pace)
        while begin < chunks - 1 and begin * pace < 4:
            prepare_chunk(begin)
            stream.run(begin * pace, (begin + 1) * pace)
            begin += 1

    def advance(c, carry):
        prepare_chunk(c)
        if pace:
            stream.run(c * pace, (c + 1) * pace)
        return carry

    lax.fori_loop(begin, chunks - 1, advance, 0)

    def wrap(i, carry):
        for f in range(6):
            for j in range(n):
                par[f, j, rows8((8 * i, FRONT - 24 * UN)), :] = par[f, j, rows8((8 * i, FRONT + rows - 24 * UN)), :]
        return carry

    lax.fori_loop(0, 3 * UN, wrap, 0)

    for i in range(2):
        for t in range(tall):
            x = packed[i, t * LANE : (t + 1) * LANE, :].T
            for f in range(8 * i, min(8 * i + 8, NF)):
                o = 16 * (f - 8 * i)
                own_r[f, t] = x[o : o + 8]
                own_l[f, t] = x[o + 8 : o + 16]
                a, g = SENT[f]
                dst = (col_va, col_sa, col_p)[a]
                dst[0, g, t, 16:24, :] = x[o + 8 : o + 16]
                dst[1, g, t, 8:16, :] = x[o : o + 8]
    up, down = zero, zero
    for i in range(2 * NF):
        src = own_l if i < NF else own_r
        g = (lane >= 4 * i) & (lane < 4 * i + 4)
        up = select(g, roll(src[i % NF, 0], 4 * i, 1), up)
        down = select(g, roll(src[i % NF, tall - 1], 4 * i + 4, 1), down)
    corner_u[...] = up
    corner_d[...] = down
    for d in DIRS[2:4]:
        @pl.when(exists(d))
        def _():
            message(d, 0)[0].start()
    for d in CORNERS:
        @pl.when(exists(d))
        def _():
            message(d, 1)[0].start()

    stream.run((chunks - 1) * pace, ITERS * blocks // UN + 3)

    def clear(ref, lead):
        for i in lead:
            ref[i] = jnp.zeros(ref.shape[1:], f32)

    for d, buf in (((-1, 0), recv_u), ((1, 0), recv_d), ((0, -1), recv_l), ((0, 1), recv_r)):
        @pl.when(~exists(d))
        def _():
            clear(buf, range(buf.shape[0]))

    for c, d in enumerate(CORNERS):
        @pl.when(~exists(d))
        def _():
            corner_in[c] = zero

    for d in DIRS:
        @pl.when(exists(d))
        def _():
            for cp in message((-d[0], -d[1]), 2):
                cp.wait_recv()
            for cp in message(d, 2):
                cp.wait_send()

    for i in range(NF):
        a, f = SENT[i]
        dst = (row_va, row_sa, row_p)[a]
        g, odd = divmod(i, 2)
        for j in range(n):
            x, y = recv_u[g, j], recv_d[g, j]
            x = roll(x, 4, 0) if odd else x
            y = y if odd else roll(y, 4, 0)
            dst[0, f, j, 8:16, :] = select(sub < 4, x, dst[0, f, j, 8:16, :])
            dst[1, f, j, 16:24, :] = select(sub < 4, dst[1, f, j, 16:24, :], y)
        dst = (col_va, col_sa, col_p)[a]
        for t in range(tall):
            dst[0, f, t, 8:16, :] = recv_l[i, t]
            dst[1, f, t, 16:24, :] = recv_r[i, t]

        def corner(u, d, at):
            x = roll(corner_in[CORNERS.index(u)], LANE - 4 - 4 * at, 1)
            y = roll(corner_in[CORNERS.index(d)], -4 * at, 1)
            return select(lane < 4, y, select(lane >= LANE - 4, x, zero))

        dst[0, f, tall, 8:16, :] = corner((-1, -1), (1, -1), NF + i)
        dst[0, f, tall, 16:24, :] = corner((-1, 0), (1, 0), i)
        dst[1, f, tall, 8:16, :] = corner((-1, 0), (1, 0), NF + i)
        dst[1, f, tall, 16:24, :] = corner((-1, 1), (1, 1), i)

    strips = []
    for s, va, vb, sa, sb, x, fr, p in (
        (sw, row_va, row_vb, row_sa, row_sb, row_x, row_f, row_p),
        (Sweep(tall + 1, True), col_va, col_vb, col_sa, col_sb, col_x, col_f, col_p),
    ):
        for i in range(2):
            strips.append((s, i, *(View(y.at[i]) for y in (va, vb, sa, sb, x, fr, p))))

    def strip_cycles(t, carry):
        for flip in (False, True):
            for s, i, va, vb, sa, sb, x, fr, p in strips:
                for k in range(2):
                    s.spread(vb if flip else va, x, k)
            for s, i, va, vb, sa, sb, x, fr, p in strips:
                for k in range(2):
                    s.stress(vb if flip else va, x, *((sb, sa) if flip else (sa, sb)), p, k)
            for s, i, va, vb, sa, sb, x, fr, p in strips:
                for k in range(2):
                    s.force(sa if flip else sb, fr, k)
            for s, i, va, vb, sa, sb, x, fr, p in strips:
                for k in range(2):
                    s.velocity(*((vb, va, sa) if flip else (va, vb, sb)), fr, p, k)
        return carry

    lax.fori_loop(0, ITERS // 2, strip_cycles, 0)
    row_e, col_e = (row_va, row_sa), (col_va, col_sa)
    sums = [[zero, zero] for _ in range(n)]
    more = [zero, zero]
    for s, i, va, vb, sa, sb, x, fr, p in strips:
        for k in range(2):
            def add(j, x, y):
                if s.turned and (j == tall or k == i):
                    return
                good = sub >= 4 if k == 0 else sub < 4
                box = more if s.turned else sums[j]
                box[0] += select(good, x, zero)
                box[1] += select(good, y, zero)

            s.reduce(vb, va, p, k, add)

    last = FRONT + ITERS * rows
    acc[...] = jnp.zeros_like(acc)

    def reduce_rows(p, group, lead):
        part = {}

        def add(j, x, y):
            for i, z in ((2 * j, x), (2 * j + 1, y)):
                part[i] = part[i] + z if i in part else z

        base = pl.multiple_of(p * (8 * group), 8 * group)
        for i in range(group):
            sw.reduce(View(ve, last - rows + lead, base), View(ve, last + lead, base), View(par, FRONT + lead, base), i, add)
        for i, z in part.items():
            acc[i] += z

    lax.fori_loop(0, (blocks - 2) // 2, lambda p, c: (reduce_rows(p, 2, 8), c)[1], 0)

    for j in range(n):
        good = lane >= 4 if j == 0 else lane < LANE - 4 if j == n - 1 else None
        if n == 1:
            good = (lane >= 4) & (lane < LANE - 4)
        for i in range(2):
            x = acc[2 * j + i] + sums[j][i]
            more[i] += x if good is None else jnp.where(good, x, 0.0)
    x, y = (jnp.sum(m, axis=0, keepdims=True) for m in more)
    x, y = x + roll(x, LANE // 2, 1), y + roll(y, LANE // 2, 1)
    half = lax.broadcasted_iota(jnp.int32, (1, LANE), 1) < LANE // 2
    part = jnp.where(half, x, y)
    mine[...] = part

    def sum_copy(x, y):
        return pltpu.make_async_remote_copy(
            src_ref=mine, dst_ref=slots.at[me], send_sem=sum_sem.at[0], recv_sem=sum_sem.at[1],
            device_id=(x, y), device_id_type=MESH,
        )

    others(lambda x, y: sum_copy(x, y).start())
    slots[pl.ds(me, 1)] = part[None]

    for t in range(tall):
        for o, (a, f) in enumerate(SENT[:5]):
            x = select(sub < 4, col_e[a][0, f, t, 16:24, :], col_e[a][1, f, t, 8:16, :])
            edge_t[t, o * 8 : o * 8 + 8, :] = roll(x, 4, 0)
    for t in range(tall):
        edge[t * LANE : (t + 1) * LANE, :] = edge_t[t].T

    def emit(rowsl, src):
        ev = edge[rowsl, :]
        es = [roll(ev, LANE - 4 - 8 * o, 1) for o in range(5)]
        for j in range(n):
            vals = [src[a][0][f, j, src[a][1], :] for a, f in SENT[:5]]
            if j == 0:
                vals = [select(lane < 4, e, x) for e, x in zip(es, vals)]
            if j == n - 1:
                vals = [select(lane >= LANE - 4, e, x) for e, x in zip(es, vals)]
            q, r, al, be, s2 = vals
            c = slice(j * LANE, (j + 1) * LANE)
            vel_out[0, rowsl, c] = 0.5 * (q + r)
            vel_out[1, rowsl, c] = 0.5 * (q - r)
            stress_out[0, rowsl, c] = 0.5 * (al + be)
            stress_out[1, rowsl, c] = s2
            stress_out[2, rowsl, c] = 0.25 * (al - be)

    def row_strip(i):
        return [(x.at[i], slice(12, 20)) for x in row_e]

    emit(slice(0, 8), row_strip(0))
    emit(slice(rows - 8, rows), row_strip(1))

    def emit_rows(base, count):
        for i in range(1, count + 1):
            at = rows8((base, 8 * i + last))
            emit(rows8((base, 8 * i)), [(ve, at), (ss, at)])

    batch = min(10, blocks - 2)

    def body(p, c):
        emit_rows(pl.multiple_of(p * (8 * batch), 8), batch)
        return c

    lax.fori_loop(0, (blocks - 2) // batch, body, 0)
    emit_rows((blocks - 2) // batch * batch * 8, (blocks - 2) % batch)

    for i in range(2):
        most = slots.at[pl.ds(0, count - 1)]
        pltpu.make_async_copy(most, most, sum_sem.at[i]).wait()
    total = [slots[i] for i in range(count)]
    while len(total) > 1:
        total = [a + b for a, b in zip(total[::2], total[1::2])] + total[len(total) // 2 * 2 :]
    total = total[0]
    scale = 1.0 / (rows * nx * cols * ny)
    x = jnp.sum(jnp.where(half, total, 0.0), axis=1, keepdims=True) * (0.5 * scale)
    y = jnp.sum(jnp.where(half, 0.0, total), axis=1, keepdims=True) * (0.0625 * scale)
    total_out[...] = jnp.where(half, x, y)


def write_kernel(vel, stress, total, new_vel, new_stress, residual, kinetic, res, kin, sem, few):
    copies = [
        pltpu.make_async_copy(a.at[f, part], b.at[f, part], sem.at[k])
        for k, (a, b) in enumerate(((vel, new_vel), (stress, new_stress)))
        for f in range(a.shape[0])
        for part in (pl.ds(0, a.shape[1] // 2), pl.ds(a.shape[1] // 2, a.shape[1] // 2))
    ]
    for c in copies:
        c.start()
    x = total[...]
    res[0, 0] = x[0, 0]
    kin[0, 0] = x[0, LANE - 1]
    copies = [pltpu.make_async_copy(a, b, few.at[i]) for i, (a, b) in enumerate(((res, residual), (kin, kinetic)))]
    for c in copies:
        c.start()
    copies += [pltpu.make_async_copy(a, b, sem.at[k]) for k, (a, b) in enumerate(((vel, new_vel), (stress, new_stress)))]
    for c in copies:
        c.wait()


def per_device(nx, ny, velocity, stress, strength, ice_mass, wind, current, ice_mask, open_water):
    _, rows, cols = velocity.shape
    n, tall, strip = cols // LANE, rows // LANE, rows + 2 * PAD
    i32 = jnp.int32
    vmem = pl.BlockSpec(memory_space=pltpu.VMEM)
    hbm = pl.BlockSpec(memory_space=pl.ANY)
    dma = pltpu.SemaphoreType.DMA
    V = pltpu.VMEM
    count = nx * ny
    new_vel, new_stress, total = pl.pallas_call(
        functools.partial(core_kernel, nx, ny, rows, cols),
        out_shape=(V((2, rows, cols), f32), V((3, rows, cols), f32), V((1, LANE), f32)),
        in_specs=[pl.BlockSpec(memory_space=pltpu.HBM)] * 8,
        out_specs=(vmem, vmem, vmem),
        scratch_shapes=[
            V((rows, cols), f32), V((rows, cols), f32), V((rows, cols), i32), V((rows, cols), i32),
            V((2, rows, cols), f32), V((2, rows, cols), f32),
            V((2, n, FRONT + (ITERS + 1) * rows + 8, LANE), f32), V((2, n, rows + PAD, LANE), f32),
            V((3, n, FRONT + (ITERS + 1) * rows + 8, LANE), f32), V((2, n, 2 * 8 * UN + PAD, LANE), f32),
            V((6, n, FRONT + rows + 8, LANE), f32), V((2 * n, 8, LANE), f32),
            V((PAIRS, n, 8, LANE), f32), V((PAIRS, n, 8, LANE), f32),
            V((PAIRS, n, 8, LANE), f32), V((PAIRS, n, 8, LANE), f32),
            V((NF, tall, 8, LANE), f32), V((NF, tall, 8, LANE), f32),
            V((NF, tall, 8, LANE), f32), V((NF, tall, 8, LANE), f32),
            V((8, LANE), f32), V((8, LANE), f32), V((6, 8, LANE), f32),
            V((2, 2, n, 32, LANE), f32), V((2, 2, n, 32, LANE), f32),
            V((2, 3, n, 32, LANE), f32), V((2, 3, n, 32, LANE), f32), V((2, 2, n, 32, LANE), f32),
            V((2, 2, n, 32, LANE), f32), V((2, 6, n, 32, LANE), f32),
            V((2, 2, tall + 1, 32, LANE), f32), V((2, 2, tall + 1, 32, LANE), f32),
            V((2, 3, tall + 1, 32, LANE), f32), V((2, 3, tall + 1, 32, LANE), f32), V((2, 2, tall + 1, 32, LANE), f32),
            V((2, 2, tall + 1, 32, LANE), f32), V((2, 6, tall + 1, 32, LANE), f32),
            V((2, rows, LANE), f32), V((tall, LANE, LANE), f32), V((rows, LANE), f32),
            V((1, LANE), f32), V((count, 1, LANE), f32),
            dma((8,)), dma((10,)), dma((10,)), dma((2,)),
        ],
        compiler_params=pltpu.CompilerParams(
            collective_id=0, has_side_effects=True, vmem_limit_bytes=57 << 20
        ),
        name="core",
    )(
        *[
            pltpu.with_memory_space_constraint(x, pltpu.HBM)
            for x in (velocity, stress, strength, ice_mass, wind, current, ice_mask, open_water)
        ]
    )
    new_vel, new_stress, residual, kinetic = pl.pallas_call(
        write_kernel,
        out_shape=(
            jax.ShapeDtypeStruct(velocity.shape, f32),
            jax.ShapeDtypeStruct(stress.shape, f32),
            jax.ShapeDtypeStruct((1, 1), f32),
            jax.ShapeDtypeStruct((1, 1), f32),
        ),
        in_specs=[vmem, vmem, vmem],
        out_specs=(hbm,) * 4,
        scratch_shapes=[pltpu.SMEM((1, 1), f32), pltpu.SMEM((1, 1), f32), dma((2,)), dma((2,))],
        compiler_params=pltpu.CompilerParams(vmem_limit_bytes=1 << 20),
        name="write",
    )(new_vel, new_stress, total)
    return new_vel, new_stress, residual.reshape(()), kinetic.reshape(())


def solution(mesh):
    two, three = P("gx", "gy"), P(None, "gx", "gy")
    return jax.shard_map(
        functools.partial(per_device, mesh.shape["gx"], mesh.shape["gy"]),
        mesh=mesh,
        in_specs=(three, three, two, two, three, three, two, two),
        out_specs=(three, three, P(), P()),
        check_vma=False,
    )
```

```python
import functools

import jax
import jax.numpy as jnp
from jax import lax
from jax.experimental import pallas as pl
from jax.experimental.pallas import tpu as pltpu
from jax.sharding import PartitionSpec as P

ITERS = 4
relax_rate = 0.8
time_step = 0.5
drag_coef = 1.0
coriolis = 0.3
delta_floor = 0.05
MESH = pl.DeviceIdType.MESH

Q, R = range(2)
AL, S2, BE = range(3)
PR, M, TQ, TR, CA, CB = range(6)
SENT = ((0, Q), (0, R), (1, AL), (1, BE), (1, S2)) + tuple((2, f) for f in range(6))
NF = len(SENT)
PAIRS = (NF + 1) // 2
LANE = 128
PAD = 8
FRONT = 128
UN = 4
DIRS = ((-1, 0), (1, 0), (0, -1), (0, 1), (-1, -1), (-1, 1), (1, -1), (1, 1))
CORNERS = ((-1, 0), (1, 0)) + DIRS[4:]
f32 = jnp.float32


def iota(axis):
    return lax.broadcasted_iota(jnp.int32, (8, LANE), axis)


def roll(x, by, axis):
    by %= x.shape[axis]
    return pltpu.roll(x, by, axis=axis) if by else x


def rows8(row):
    if isinstance(row, int):
        return slice(row, row + 8)
    base, off = row
    return pl.ds(base + off if off % 8 else pl.multiple_of(base + off, 8), 8)


def select(mask, x, y):
    return lax.select(mask, x, y)


def shift(xs, by, first, last):
    n = len(xs)
    turned = [roll(x, by, 1) for x in xs]
    if by > 0:
        return [select(first, turned[(j - 1) % n], turned[j]) for j in range(n)]
    return [select(last, turned[(j + 1) % n], turned[j]) for j in range(n)]


class View:
    def __init__(self, ref, pad=PAD, base=None):
        self.ref, self.pad, self.base = ref, pad, base

    def at(self, i, off=0):
        row = self.pad + 8 * i + off
        return rows8(row if self.base is None else (self.base, row))

    def load(self, f, j, i, off=0):
        return self.ref[f, j, self.at(i, off), :]

    def store(self, f, j, i, x):
        self.ref[f, j, self.at(i), :] = x


class Sweep:
    def __init__(self, tiles, turned):
        self.n, self.turned = tiles, turned
        self.first, self.last = iota(1) == 0, iota(1) == LANE - 1

    def spread(self, ve, vx, i):
        for f in (Q, R):
            xs = shift([ve.load(f, j, i) for j in range(self.n)], 1, self.first, self.last)
            for j, x in enumerate(xs):
                vx.store(f, j, i, x)

    def stress(self, ve, vx, old, new, par, i):
        keep = 1.0 / (1.0 + relax_rate)
        for j in range(self.n):
            q, r, qx, rx = (v.load(f, j, i) for v in (ve, vx) for f in (Q, R))
            qa, ra, qxa, rxa = (v.load(f, j, i, -1) for v in (ve, vx) for f in (Q, R))
            a, b = q - qxa, rx - ra
            if self.turned:
                d, s = a - b, a + b
                t = (r - rxa) - (qx - qa)
            else:
                d, s = a + b, a - b
                t = (r - rxa) + (qx - qa)
            e = (d * d + 4.0 * delta_floor * delta_floor) + 0.25 * (t * t + s * s)
            pr = par.load(PR, j, i)
            g = pr * lax.rsqrt(e)
            h = 0.25 * g
            push, side = g * d - pr, h * s
            new.store(AL, j, i, old.load(AL, j, i) * keep + (push + side))
            new.store(BE, j, i, old.load(BE, j, i) * keep + (push - side))
            new.store(S2, j, i, old.load(S2, j, i) * keep + h * t)

    def force(self, ss, frc, i):
        a, c = [], []
        for j in range(self.n):
            ad, s, sd, b = ss.load(AL, j, i, 1), ss.load(S2, j, i), ss.load(S2, j, i, 1), ss.load(BE, j, i)
            if self.turned:
                a.append(ad + s)
                c.append(sd + b)
            else:
                a.append(ad - s)
                c.append(sd - b)
        for f, xs in ((0, a), (1, c)):
            for j, x in enumerate(shift(xs, -1, self.first, self.last)):
                frc.store(f, j, i, x)

    def velocity(self, old, new, ss, frc, par, i):
        for j in range(self.n):
            al, s, sd, bd = ss.load(AL, j, i), ss.load(S2, j, i), ss.load(S2, j, i, 1), ss.load(BE, j, i, 1)
            fa, fc = frc.load(0, j, i), frc.load(1, j, i)
            if self.turned:
                fq, fr = fa - (sd + al), fc - (bd + s)
            else:
                fq, fr = fa + (sd - al), fc + (bd - s)
            q, r, m = old.load(Q, j, i), old.load(R, j, i), par.load(M, j, i)
            x = m * q + (fq + par.load(TQ, j, i))
            y = m * r + (fr + par.load(TR, j, i))
            ca, cb = par.load(CA, j, i), par.load(CB, j, i)
            new.store(Q, j, i, ca * x - cb * y)
            new.store(R, j, i, ca * y + cb * x)

    def reduce(self, old, new, par, i, add):
        for j in range(self.n):
            nq, nr = new.load(Q, j, i), new.load(R, j, i)
            dq, dr = nq - old.load(Q, j, i), nr - old.load(R, j, i)
            add(j, dq * dq + dr * dr, par.load(M, j, i) * (nq * nq + nr * nr))


class Stream:
    def __init__(self, sw, ve, vx, ss, frc, par, rows):
        self.sw, self.ve, self.vx, self.ss, self.frc, self.par, self.rows = sw, ve, vx, ss, frc, par, rows

    def step(self, p, stages):
        sw, rows, unit = self.sw, self.rows, 8 * UN
        row = pl.multiple_of(p * unit, unit)
        turn = pl.multiple_of(lax.rem(row, rows), unit)
        late = pl.multiple_of(lax.rem(row + rows - 4 * unit, rows), unit)
        slots = [View(self.frc, PAD, pl.multiple_of(lax.rem(p + k, 2) * unit, unit)) for k in (0, 1)]
        was = lambda ref, lag: View(ref, FRONT - lag * unit, row)
        now = lambda ref, lag: View(ref, FRONT + rows - lag * unit, row)
        par = lambda lag: View(self.par, FRONT - lag * unit, turn)
        ve, ss = self.ve, self.ss
        todo = {
            "velocity": (was(ve, 3), now(ve, 3), now(ss, 3), slots[1], par(3)),
            "force": (now(ss, 2), slots[0]),
            "stress": (was(ve, 0), View(self.vx, PAD, turn), was(ss, 0), now(ss, 0), par(0)),
            "spread": (now(ve, 4), View(self.vx, PAD, late)),
        }
        for name in stages:
            for i in range(UN):
                getattr(sw, name)(*todo[name], i)

    def run(self, lo, hi):
        every = ("velocity", "force", "stress", "spread")
        steps = ITERS * self.rows // (8 * UN)
        for a, b, stages in (
            (0, 2, every[2:3]), (2, 3, every[1:3]), (3, 4, every[:3]),
            (4, steps, every), (steps, steps + 2, every[:2]), (steps + 2, steps + 3, every[:1]),
        ):
            if isinstance(lo, int):
                a, b = max(a, lo), min(b, hi)
                if a >= b:
                    continue
            elif a != 4:
                continue
            else:
                a, b = lo, hi

            def body(p, carry):
                self.step(p, stages)
                return carry

            lax.fori_loop(a, b, body, 0)


def core_kernel(
    nx, ny, rows, cols,
    vel, stress, strength, mass, wind, current, mask, water,
    vel_out, stress_out, total_out,
    strength_v, mass_v, mask_v, water_v, wind_v, current_v,
    ve, vx, ss, frc, par, acc,
    pack_u, pack_d, recv_u, recv_d, own_l, own_r, recv_l, recv_r,
    corner_u, corner_d, corner_in,
    row_va, row_vb, row_sa, row_sb, row_x, row_f, row_p, col_va, col_vb, col_sa, col_sb, col_x, col_f, col_p,
    packed, edge_t, edge, mine, slots,
    load_sem, send_sem, recv_sem, sum_sem,
):
    ix = lax.axis_index("gx")
    iy = lax.axis_index("gy")
    n, tall, blocks = cols // LANE, rows // LANE, rows // 8
    chunks = 8
    per = rows // chunks
    lane, sub = iota(1), iota(0)
    zero = jnp.zeros((8, LANE), f32)

    def loads(c):
        part = pl.ds(pl.multiple_of(c * per, 8), per)
        later = pl.ds(pl.multiple_of(c * per + FRONT, 8), per)
        both = slice(None)
        pairs = [
            (strength.at[part], strength_v.at[part]),
            (mass.at[part], mass_v.at[part]),
            (mask.at[part], mask_v.at[part]),
            (water.at[part], water_v.at[part]),
            (wind.at[both, part], wind_v.at[both, part]),
            (current.at[both, part], current_v.at[both, part]),
        ]
        for j in range(n):
            tile = pl.ds(j * LANE, LANE)
            pairs.append((vel.at[both, part, tile], ve.at[both, j, later]))
            pairs.append((stress.at[both, part, tile], ss.at[both, j, later]))
        return [pltpu.make_async_copy(a, b, load_sem.at[c]) for a, b in pairs]

    for c in range(chunks):
        for cp in loads(c):
            cp.start()

    count = nx * ny
    me = ix * ny + iy

    def others(act):
        xs = [lax.rem(ix + nx // 2 + k, nx) for k in range(nx)]
        ys = [lax.rem(iy + ny // 2 + k, ny) for k in range(ny)]
        for i, x in enumerate(xs):
            for j, y in enumerate(ys):
                if (nx // 2 + i) % nx or (ny // 2 + j) % ny:
                    act(x, y)

    barrier = pltpu.get_barrier_semaphore()
    others(lambda x, y: pl.semaphore_signal(barrier, inc=1, device_id=(x, y), device_id_type=MESH))

    for j in range(n):
        for f in range(2):
            ve[f, j, FRONT - 8 : FRONT, :] = zero
            vx[f, j, 0:8, :] = zero
        for f in range(3):
            ss[f, j, FRONT + (ITERS + 1) * rows : FRONT + (ITERS + 1) * rows + 8, :] = zero
    for st in (row_va, row_vb, row_sa, row_sb, row_x, col_va, col_vb, col_sa, col_sb, col_x):
        for side in range(2):
            for f in range(st.shape[1]):
                for j in range(st.shape[2]):
                    st[side, f, j, 0:8, :] = zero
                    st[side, f, j, 24:32, :] = zero

    sw = Sweep(n, False)

    def prepare(base, i):
        rowsl, at = rows8((base, 8 * i)), rows8((base, 8 * i + FRONT))
        ends = []
        for j in range(n):
            src = (rowsl, slice(j * LANE, (j + 1) * LANE))
            w = mask_v[src].astype(f32) * (1.0 - water_v[src].astype(f32))
            m = mass_v[src]
            inertia = m * (1.0 / time_step)
            diagonal = inertia + drag_coef
            turning = m * coriolis
            scale = (0.5 * w) / (diagonal * diagonal + turning * turning)
            tx = wind_v[(0,) + src] + drag_coef * current_v[(0,) + src]
            ty = wind_v[(1,) + src] + drag_coef * current_v[(1,) + src]
            u, v = ve[0, j, at, :], ve[1, j, at, :]
            s1, s2, s12 = (ss[f, j, at, :] for f in range(3))
            t = s12 + s12
            q, r = u + v, u - v
            moving = {Q: q, R: r}
            state = {AL: s1 + t, BE: s1 - t, S2: s2}
            fixed = {
                PR: strength_v[src] * w * (relax_rate / (1.0 + relax_rate)),
                M: inertia * 2.0,
                TQ: (tx + ty) * 2.0,
                TR: (tx - ty) * 2.0,
                CA: diagonal * scale,
                CB: turning * scale,
            }
            for f, x in moving.items():
                ve[f, j, at, :] = x
            for f, x in ((AL, state[AL]), (BE, state[BE])):
                ss[f, j, at, :] = x
            for f, x in fixed.items():
                par[f, j, at, :] = x
            if j in (0, n - 1):
                ends.append([(moving, state, fixed)[a][f] for a, f in SENT])
        low, high = ends[0], ends[-1]
        packs = [zero, zero]
        for i in range(NF):
            x = roll(select(lane < LANE // 2, low[i], high[i]), 16 * (i % 8) + 8, 1)
            g = (lane >= 16 * (i % 8)) & (lane < 16 * (i % 8) + 16)
            packs[i // 8] = select(g, x, packs[i // 8])
        for i in range(2):
            packed[i, rowsl, :] = packs[i]

    group = min(8, per // 8)

    def prepare_chunk(c):
        size = ve.at[0, :, pl.ds(0, 13 * per)]
        pltpu.make_async_copy(size, size, load_sem.at[c]).wait()

        def body(p, carry):
            base = pl.multiple_of(c * per + p * (8 * group), 8 * group)
            for i in range(group):
                prepare(base, i)
            for i in range(group):
                sw.spread(View(ve, FRONT, base), View(vx, PAD, base), i)
            return carry

        lax.fori_loop(0, per // 8 // group, body, 0)

    def exists(d):
        return (ix + d[0] >= 0) & (ix + d[0] < nx) & (iy + d[1] >= 0) & (iy + d[1] < ny)

    def message(d, which):
        k = DIRS.index(d)
        dx, dy = d
        out = []
        if which == 1:
            pass
        elif dy == 0:
            out.append((pack_u, recv_d, k) if dx < 0 else (pack_d, recv_u, k))
        elif dx == 0:
            out.append((own_l, recv_r, k) if dy < 0 else (own_r, recv_l, k))
        if dx and which != 0:
            c = CORNERS.index(d)
            back = CORNERS.index((-dx, -dy))
            out.append((corner_u if dx < 0 else corner_d, corner_in.at[back], 4 + c))
        return [
            pltpu.make_async_remote_copy(
                src_ref=a, dst_ref=b, send_sem=send_sem.at[s], recv_sem=recv_sem.at[s],
                device_id=(ix + dx, iy + dy), device_id_type=MESH,
            )
            for a, b, s in out
        ]

    def plane(i, j, block):
        a, f = SENT[i]
        row = block * 8 + FRONT
        return (ve, ss, par)[a][f, j, row : row + 8, :]

    stream = Stream(sw, ve, vx, ss, frc, par, rows)
    pace = per // (8 * UN)
    begin = 1
    prepare_chunk(0)
    if pace:
        stream.run(0, pace)
        while begin < chunks and begin * pace < 4:
            prepare_chunk(begin)
            stream.run(begin * pace, (begin + 1) * pace)
            begin += 1

    def advance(c, carry):
        prepare_chunk(c)
        if pace:
            stream.run(c * pace, (c + 1) * pace)
        return carry

    lax.fori_loop(begin, chunks, advance, 0)

    def wrap(i, carry):
        for f in range(6):
            for j in range(n):
                par[f, j, rows8((8 * i, FRONT - 24 * UN)), :] = par[f, j, rows8((8 * i, FRONT + rows - 24 * UN)), :]
        return carry

    lax.fori_loop(0, 3 * UN, wrap, 0)

    for g in range(PAIRS):
        i0, i1 = 2 * g, min(2 * g + 1, NF - 1)
        for j in range(n):
            pack_u[g, j] = select(sub < 4, plane(i0, j, 0), roll(plane(i1, j, 0), 4, 0))
            pack_d[g, j] = select(sub < 4, roll(plane(i0, j, blocks - 1), 4, 0), plane(i1, j, blocks - 1))

    for i in range(NF):
        a, f = SENT[i]
        dst = (row_va, row_sa, row_p)[a]
        for j in range(n):
            x, y = (roll(plane(i, j, b), 4, 0) for b in (0, 1))
            dst[0, f, j, 8:16, :] = x
            dst[0, f, j, 16:24, :] = select(sub < 4, x, y)
            x, y = (roll(plane(i, j, b), 4, 0) for b in (blocks - 2, blocks - 1))
            dst[1, f, j, 8:16, :] = select(sub < 4, x, y)
            dst[1, f, j, 16:24, :] = y

    pl.semaphore_wait(barrier, count - 1)
    for d in DIRS[:2]:
        @pl.when(exists(d))
        def _():
            message(d, 0)[0].start()

    for i in range(2):
        for t in range(tall):
            x = packed[i, t * LANE : (t + 1) * LANE, :].T
            for f in range(8 * i, min(8 * i + 8, NF)):
                o = 16 * (f - 8 * i)
                own_r[f, t] = x[o : o + 8]
                own_l[f, t] = x[o + 8 : o + 16]
                a, g = SENT[f]
                dst = (col_va, col_sa, col_p)[a]
                dst[0, g, t, 16:24, :] = x[o + 8 : o + 16]
                dst[1, g, t, 8:16, :] = x[o : o + 8]
    up, down = zero, zero
    for i in range(2 * NF):
        src = own_l if i < NF else own_r
        g = (lane >= 4 * i) & (lane < 4 * i + 4)
        up = select(g, roll(src[i % NF, 0], 4 * i, 1), up)
        down = select(g, roll(src[i % NF, tall - 1], 4 * i + 4, 1), down)
    corner_u[...] = up
    corner_d[...] = down
    for d in DIRS[2:4]:
        @pl.when(exists(d))
        def _():
            message(d, 0)[0].start()
    for d in CORNERS:
        @pl.when(exists(d))
        def _():
            message(d, 1)[0].start()

    stream.run(chunks * pace, ITERS * blocks // UN + 3)

    last = FRONT + ITERS * rows
    acc[...] = jnp.zeros_like(acc)

    def reduce_rows(p, group, lead):
        part = {}

        def add(j, x, y):
            for i, z in ((2 * j, x), (2 * j + 1, y)):
                part[i] = part[i] + z if i in part else z

        base = pl.multiple_of(p * (8 * group), 8 * group)
        for i in range(group):
            sw.reduce(View(ve, last - rows + lead, base), View(ve, last + lead, base), View(par, FRONT + lead, base), i, add)
        for i, z in part.items():
            acc[i] += z

    lax.fori_loop(0, (blocks - 2) // 2, lambda p, c: (reduce_rows(p, 2, 8), c)[1], 0)

    def clear(ref, lead):
        for i in lead:
            ref[i] = jnp.zeros(ref.shape[1:], f32)

    for d, buf in (((-1, 0), recv_u), ((1, 0), recv_d), ((0, -1), recv_l), ((0, 1), recv_r)):
        @pl.when(~exists(d))
        def _():
            clear(buf, range(buf.shape[0]))

    for c, d in enumerate(CORNERS):
        @pl.when(~exists(d))
        def _():
            corner_in[c] = zero

    for d in DIRS:
        @pl.when(exists(d))
        def _():
            for cp in message((-d[0], -d[1]), 2):
                cp.wait_recv()
            for cp in message(d, 2):
                cp.wait_send()

    for i in range(NF):
        a, f = SENT[i]
        dst = (row_va, row_sa, row_p)[a]
        g, odd = divmod(i, 2)
        for j in range(n):
            x, y = recv_u[g, j], recv_d[g, j]
            x = roll(x, 4, 0) if odd else x
            y = y if odd else roll(y, 4, 0)
            dst[0, f, j, 8:16, :] = select(sub < 4, x, dst[0, f, j, 8:16, :])
            dst[1, f, j, 16:24, :] = select(sub < 4, dst[1, f, j, 16:24, :], y)
        dst = (col_va, col_sa, col_p)[a]
        for t in range(tall):
            dst[0, f, t, 8:16, :] = recv_l[i, t]
            dst[1, f, t, 16:24, :] = recv_r[i, t]

        def corner(u, d, at):
            x = roll(corner_in[CORNERS.index(u)], LANE - 4 - 4 * at, 1)
            y = roll(corner_in[CORNERS.index(d)], -4 * at, 1)
            return select(lane < 4, y, select(lane >= LANE - 4, x, zero))

        dst[0, f, tall, 8:16, :] = corner((-1, -1), (1, -1), NF + i)
        dst[0, f, tall, 16:24, :] = corner((-1, 0), (1, 0), i)
        dst[1, f, tall, 8:16, :] = corner((-1, 0), (1, 0), NF + i)
        dst[1, f, tall, 16:24, :] = corner((-1, 1), (1, 1), i)

    strips = []
    for s, va, vb, sa, sb, x, fr, p in (
        (sw, row_va, row_vb, row_sa, row_sb, row_x, row_f, row_p),
        (Sweep(tall + 1, True), col_va, col_vb, col_sa, col_sb, col_x, col_f, col_p),
    ):
        for i in range(2):
            strips.append((s, i, *(View(y.at[i]) for y in (va, vb, sa, sb, x, fr, p))))

    def strip_cycles(t, carry):
        for flip in (False, True):
            for s, i, va, vb, sa, sb, x, fr, p in strips:
                for k in range(2):
                    s.spread(vb if flip else va, x, k)
            for s, i, va, vb, sa, sb, x, fr, p in strips:
                for k in range(2):
                    s.stress(vb if flip else va, x, *((sb, sa) if flip else (sa, sb)), p, k)
            for s, i, va, vb, sa, sb, x, fr, p in strips:
                for k in range(2):
                    s.force(sa if flip else sb, fr, k)
            for s, i, va, vb, sa, sb, x, fr, p in strips:
                for k in range(2):
                    s.velocity(*((vb, va, sa) if flip else (va, vb, sb)), fr, p, k)
        return carry

    lax.fori_loop(0, ITERS // 2, strip_cycles, 0)
    row_e, col_e = (row_va, row_sa), (col_va, col_sa)
    sums = [[zero, zero] for _ in range(n)]
    more = [zero, zero]
    for s, i, va, vb, sa, sb, x, fr, p in strips:
        for k in range(2):
            def add(j, x, y):
                if s.turned and (j == tall or k == i):
                    return
                good = sub >= 4 if k == 0 else sub < 4
                box = more if s.turned else sums[j]
                box[0] += select(good, x, zero)
                box[1] += select(good, y, zero)

            s.reduce(vb, va, p, k, add)

    for j in range(n):
        good = lane >= 4 if j == 0 else lane < LANE - 4 if j == n - 1 else None
        if n == 1:
            good = (lane >= 4) & (lane < LANE - 4)
        for i in range(2):
            x = acc[2 * j + i] + sums[j][i]
            more[i] += x if good is None else jnp.where(good, x, 0.0)
    x, y = (jnp.sum(m, axis=0, keepdims=True) for m in more)
    x, y = x + roll(x, LANE // 2, 1), y + roll(y, LANE // 2, 1)
    half = lax.broadcasted_iota(jnp.int32, (1, LANE), 1) < LANE // 2
    part = jnp.where(half, x, y)
    mine[...] = part

    def sum_copy(x, y):
        return pltpu.make_async_remote_copy(
            src_ref=mine, dst_ref=slots.at[me], send_sem=sum_sem.at[0], recv_sem=sum_sem.at[1],
            device_id=(x, y), device_id_type=MESH,
        )

    others(lambda x, y: sum_copy(x, y).start())
    slots[pl.ds(me, 1)] = part[None]

    for t in range(tall):
        for o, (a, f) in enumerate(SENT[:5]):
            x = select(sub < 4, col_e[a][0, f, t, 16:24, :], col_e[a][1, f, t, 8:16, :])
            edge_t[t, o * 8 : o * 8 + 8, :] = roll(x, 4, 0)
    for t in range(tall):
        edge[t * LANE : (t + 1) * LANE, :] = edge_t[t].T

    def emit(rowsl, src):
        ev = edge[rowsl, :]
        es = [roll(ev, LANE - 4 - 8 * o, 1) for o in range(5)]
        for j in range(n):
            vals = [src[a][0][f, j, src[a][1], :] for a, f in SENT[:5]]
            if j == 0:
                vals = [select(lane < 4, e, x) for e, x in zip(es, vals)]
            if j == n - 1:
                vals = [select(lane >= LANE - 4, e, x) for e, x in zip(es, vals)]
            q, r, al, be, s2 = vals
            c = slice(j * LANE, (j + 1) * LANE)
            vel_out[0, rowsl, c] = 0.5 * (q + r)
            vel_out[1, rowsl, c] = 0.5 * (q - r)
            stress_out[0, rowsl, c] = 0.5 * (al + be)
            stress_out[1, rowsl, c] = s2
            stress_out[2, rowsl, c] = 0.25 * (al - be)

    def row_strip(i):
        return [(x.at[i], slice(12, 20)) for x in row_e]

    emit(slice(0, 8), row_strip(0))
    emit(slice(rows - 8, rows), row_strip(1))

    def emit_rows(base, count):
        for i in range(1, count + 1):
            at = rows8((base, 8 * i + last))
            emit(rows8((base, 8 * i)), [(ve, at), (ss, at)])

    batch = min(10, blocks - 2)

    def body(p, c):
        emit_rows(pl.multiple_of(p * (8 * batch), 8), batch)
        return c

    lax.fori_loop(0, (blocks - 2) // batch, body, 0)
    emit_rows((blocks - 2) // batch * batch * 8, (blocks - 2) % batch)

    for i in range(2):
        most = slots.at[pl.ds(0, count - 1)]
        pltpu.make_async_copy(most, most, sum_sem.at[i]).wait()
    total = [slots[i] for i in range(count)]
    while len(total) > 1:
        total = [a + b for a, b in zip(total[::2], total[1::2])] + total[len(total) // 2 * 2 :]
    total = total[0]
    scale = 1.0 / (rows * nx * cols * ny)
    x = jnp.sum(jnp.where(half, total, 0.0), axis=1, keepdims=True) * (0.5 * scale)
    y = jnp.sum(jnp.where(half, 0.0, total), axis=1, keepdims=True) * (0.0625 * scale)
    total_out[...] = jnp.where(half, x, y)


def write_kernel(vel, stress, total, new_vel, new_stress, residual, kinetic, res, kin, sem, few):
    copies = [
        pltpu.make_async_copy(a.at[f, part], b.at[f, part], sem.at[k])
        for k, (a, b) in enumerate(((vel, new_vel), (stress, new_stress)))
        for f in range(a.shape[0])
        for part in (pl.ds(0, a.shape[1] // 2), pl.ds(a.shape[1] // 2, a.shape[1] // 2))
    ]
    for c in copies:
        c.start()
    x = total[...]
    res[0, 0] = x[0, 0]
    kin[0, 0] = x[0, LANE - 1]
    copies = [pltpu.make_async_copy(a, b, few.at[i]) for i, (a, b) in enumerate(((res, residual), (kin, kinetic)))]
    for c in copies:
        c.start()
    copies += [pltpu.make_async_copy(a, b, sem.at[k]) for k, (a, b) in enumerate(((vel, new_vel), (stress, new_stress)))]
    for c in copies:
        c.wait()


def per_device(nx, ny, velocity, stress, strength, ice_mass, wind, current, ice_mask, open_water):
    _, rows, cols = velocity.shape
    n, tall, strip = cols // LANE, rows // LANE, rows + 2 * PAD
    i32 = jnp.int32
    vmem = pl.BlockSpec(memory_space=pltpu.VMEM)
    hbm = pl.BlockSpec(memory_space=pl.ANY)
    dma = pltpu.SemaphoreType.DMA
    V = pltpu.VMEM
    count = nx * ny
    new_vel, new_stress, total = pl.pallas_call(
        functools.partial(core_kernel, nx, ny, rows, cols),
        out_shape=(V((2, rows, cols), f32), V((3, rows, cols), f32), V((1, LANE), f32)),
        in_specs=[pl.BlockSpec(memory_space=pltpu.HBM)] * 8,
        out_specs=(vmem, vmem, vmem),
        scratch_shapes=[
            V((rows, cols), f32), V((rows, cols), f32), V((rows, cols), i32), V((rows, cols), i32),
            V((2, rows, cols), f32), V((2, rows, cols), f32),
            V((2, n, FRONT + (ITERS + 1) * rows + 8, LANE), f32), V((2, n, rows + PAD, LANE), f32),
            V((3, n, FRONT + (ITERS + 1) * rows + 8, LANE), f32), V((2, n, 2 * 8 * UN + PAD, LANE), f32),
            V((6, n, FRONT + rows + 8, LANE), f32), V((2 * n, 8, LANE), f32),
            V((PAIRS, n, 8, LANE), f32), V((PAIRS, n, 8, LANE), f32),
            V((PAIRS, n, 8, LANE), f32), V((PAIRS, n, 8, LANE), f32),
            V((NF, tall, 8, LANE), f32), V((NF, tall, 8, LANE), f32),
            V((NF, tall, 8, LANE), f32), V((NF, tall, 8, LANE), f32),
            V((8, LANE), f32), V((8, LANE), f32), V((6, 8, LANE), f32),
            V((2, 2, n, 32, LANE), f32), V((2, 2, n, 32, LANE), f32),
            V((2, 3, n, 32, LANE), f32), V((2, 3, n, 32, LANE), f32), V((2, 2, n, 32, LANE), f32),
            V((2, 2, n, 32, LANE), f32), V((2, 6, n, 32, LANE), f32),
            V((2, 2, tall + 1, 32, LANE), f32), V((2, 2, tall + 1, 32, LANE), f32),
            V((2, 3, tall + 1, 32, LANE), f32), V((2, 3, tall + 1, 32, LANE), f32), V((2, 2, tall + 1, 32, LANE), f32),
            V((2, 2, tall + 1, 32, LANE), f32), V((2, 6, tall + 1, 32, LANE), f32),
            V((2, rows, LANE), f32), V((tall, LANE, LANE), f32), V((rows, LANE), f32),
            V((1, LANE), f32), V((count, 1, LANE), f32),
            dma((8,)), dma((10,)), dma((10,)), dma((2,)),
        ],
        compiler_params=pltpu.CompilerParams(
            collective_id=0, has_side_effects=True, vmem_limit_bytes=57 << 20
        ),
        name="core",
    )(
        *[
            pltpu.with_memory_space_constraint(x, pltpu.HBM)
            for x in (velocity, stress, strength, ice_mass, wind, current, ice_mask, open_water)
        ]
    )
    new_vel, new_stress, residual, kinetic = pl.pallas_call(
        write_kernel,
        out_shape=(
            jax.ShapeDtypeStruct(velocity.shape, f32),
            jax.ShapeDtypeStruct(stress.shape, f32),
            jax.ShapeDtypeStruct((1, 1), f32),
            jax.ShapeDtypeStruct((1, 1), f32),
        ),
        in_specs=[vmem, vmem, vmem],
        out_specs=(hbm,) * 4,
        scratch_shapes=[pltpu.SMEM((1, 1), f32), pltpu.SMEM((1, 1), f32), dma((2,)), dma((2,))],
        compiler_params=pltpu.CompilerParams(vmem_limit_bytes=1 << 20),
        name="write",
    )(new_vel, new_stress, total)
    return new_vel, new_stress, residual.reshape(()), kinetic.reshape(())


def solution(mesh):
    two, three = P("gx", "gy"), P(None, "gx", "gy")
    return jax.shard_map(
        functools.partial(per_device, mesh.shape["gx"], mesh.shape["gy"]),
        mesh=mesh,
        in_specs=(three, three, two, two, three, three, two, two),
        out_specs=(three, three, P(), P()),
        check_vma=False,
    )
```
